128 devices in a mesh: fsdp: 128 (over z, y, x, core).
Axes of the slice: x: 4, y: 4, z: 4, core: 2. Of those that a mesh axis runs over, the one named last changes fastest.
Arguments:
- x_saved: bfloat16 [2, 2, 128, 1024, 512], P(None, None, 'fsdp')
- grad_out: bfloat16 [2, 128, 1024, 512], P(None, 'fsdp')
- x_next: bfloat16 [2, 128, 1024, 512], P(None, 'fsdp')
- w_up: bfloat16 [2, 2, 512, 2048], replicated
- w_down: bfloat16 [2, 2, 2048, 512], replicated
- acc_up: float32 [2, 2, 512, 2048], P(None, None, 'fsdp')
- acc_down: float32 [2, 2, 2048, 512], P(None, None, 'fsdp')
- master_up: float32 [2, 2, 512, 2048], P(None, None, 'fsdp')
- master_down: float32 [2, 2, 2048, 512], P(None, None, 'fsdp')
- moment1_up: float32 [2, 2, 512, 2048], P(None, None, 'fsdp')
- moment1_down: float32 [2, 2, 2048, 512], P(None, None, 'fsdp')
- moment2_up: float32 [2, 2, 512, 2048], P(None, None, 'fsdp')
- moment2_down: float32 [2, 2, 2048, 512], P(None, None, 'fsdp')
Outputs:
- output 1: float32 [2, 2, 512, 2048], P(None, None, 'fsdp')
- output 2: float32 [2, 2, 2048, 512], P(None, None, 'fsdp')
- output 3: float32 [2, 2, 512, 2048], P(None, None, 'fsdp')
- output 4: float32 [2, 2, 2048, 512], P(None, None, 'fsdp')
- output 5: float32 [2, 2, 512, 2048], P(None, None, 'fsdp')
- output 6: float32 [2, 2, 2048, 512], P(None, None, 'fsdp')
- output 7: bfloat16 [2, 128, 1024, 512], P(None, 'fsdp')
All inputs are finite; a program needn't handle non-finite values.
Results may differ from the reference program's by a relative error of at most 0.00795546.
Values are sent between devices in bfloat16 or wider.
A program may use at most 1 GiB of HBM per device.

```python
import functools
import jax
import jax.numpy as jnp
from jax import lax

D = 512
FF = 2048
BATCH = 128
SEQ_LEN = 1024
GROUPS = 128
STAGES = 2
LAYERS = 2
MICROBATCHES = 2
ADAM_STEP = 2
TOKENS = BATCH // GROUPS * SEQ_LEN
LEARN_RATE = 0.005
BETA_ONE = 0.9
BETA_TWO = 0.95
ADAM_EPS = 1e-8
WEIGHT_DECAY = 0.1


def setup_inputs(seed: int = 0) -> dict:
    key_list = jax.random.split(jax.random.key(seed), 13)
    row_count = BATCH * SEQ_LEN
    scale_up = 0.3 * row_count ** 0.5
    scale_down = 0.7 * row_count ** 0.5
    tok_shape = (STAGES, BATCH, SEQ_LEN, D)
    up_shape = (STAGES, LAYERS, D, FF)
    down_shape = (STAGES, LAYERS, FF, D)
    x_saved = jax.random.normal(key_list[0], (STAGES, LAYERS, BATCH, SEQ_LEN, D), jnp.float32).astype(jnp.bfloat16)
    grad_out = jax.random.normal(key_list[1], tok_shape, jnp.float32).astype(jnp.bfloat16)
    x_next = jax.random.normal(key_list[2], tok_shape, jnp.float32).astype(jnp.bfloat16)
    w_up = (jax.random.normal(key_list[3], up_shape, jnp.float32) * D ** -0.5).astype(jnp.bfloat16)
    w_down = (jax.random.normal(key_list[4], down_shape, jnp.float32) * FF ** -0.5).astype(jnp.bfloat16)
    acc_up = jax.random.normal(key_list[5], up_shape, jnp.float32) * scale_up
    acc_down = jax.random.normal(key_list[6], down_shape, jnp.float32) * scale_down
    master_up = jax.random.normal(key_list[7], up_shape, jnp.float32) * D ** -0.5
    master_down = jax.random.normal(key_list[8], down_shape, jnp.float32) * FF ** -0.5
    moment1_up = jax.random.normal(key_list[9], up_shape, jnp.float32) * (0.05 * scale_up)
    moment1_down = jax.random.normal(key_list[10], down_shape, jnp.float32) * (0.05 * scale_down)
    moment2_up = jax.random.uniform(key_list[11], up_shape, jnp.float32, 0.02, 0.06) * scale_up ** 2
    moment2_down = jax.random.uniform(key_list[12], down_shape, jnp.float32, 0.02, 0.06) * scale_down ** 2
    return {'x_saved': x_saved, 'grad_out': grad_out, 'x_next': x_next, 'w_up': w_up, 'w_down': w_down, 'acc_up': acc_up, 'acc_down': acc_down, 'master_up': master_up, 'master_down': master_down, 'moment1_up': moment1_up, 'moment1_down': moment1_down, 'moment2_up': moment2_up, 'moment2_down': moment2_down}


def backward_layer(x_in, cotangent, w_one, w_two):
    hidden = jnp.dot(x_in, w_one, preferred_element_type=jnp.float32)
    gelu_out, gelu_vjp = jax.vjp(jax.nn.gelu, hidden)
    gelu_out = gelu_out.astype(jnp.bfloat16)
    grad_act = jnp.dot(cotangent, w_two.T, preferred_element_type=jnp.float32)
    grad_hidden = gelu_vjp(grad_act)[0].astype(jnp.bfloat16)
    part_down = jnp.dot(gelu_out.T, cotangent, preferred_element_type=jnp.float32)
    part_up = jnp.dot(x_in.T, grad_hidden, preferred_element_type=jnp.float32)
    return part_up, part_down, grad_hidden


def stage_grads(x_layers, grad_top, up_stack, down_stack):
    x_blocks = jnp.swapaxes(x_layers.reshape(LAYERS, GROUPS, TOKENS, D), 0, 1)
    grad_blocks = grad_top.reshape(GROUPS, TOKENS, D)

    def scan_body(carry, block_pair):
        sum_up, sum_down = carry
        x_block, cotangent = block_pair
        up_parts = [None] * LAYERS
        down_parts = [None] * LAYERS
        for layer_id in reversed(range(LAYERS)):
            part_up, part_down, grad_hidden = backward_layer(x_block[layer_id], cotangent, up_stack[layer_id], down_stack[layer_id])
            up_parts[layer_id] = part_up
            down_parts[layer_id] = part_down
            if layer_id > 0:
                cotangent = (cotangent.astype(jnp.float32) + jnp.dot(grad_hidden, up_stack[layer_id].T, preferred_element_type=jnp.float32)).astype(jnp.bfloat16)
        return (sum_up + jnp.stack(up_parts), sum_down + jnp.stack(down_parts)), None

    start_sums = (jnp.zeros((LAYERS, D, FF), jnp.float32), jnp.zeros((LAYERS, FF, D), jnp.float32))
    final_sums, scan_rest = lax.scan(scan_body, start_sums, (x_blocks, grad_blocks))
    return final_sums


def adam_update(acc_part, grad_new, master, moment_one, moment_two):
    grad_mean = (acc_part + grad_new) / MICROBATCHES
    moment_one = BETA_ONE * moment_one + (1.0 - BETA_ONE) * grad_mean
    moment_two = BETA_TWO * moment_two + (1.0 - BETA_TWO) * grad_mean * grad_mean
    corr_one = 1.0 - BETA_ONE ** ADAM_STEP
    corr_two = 1.0 - BETA_TWO ** ADAM_STEP
    step_dir = (moment_one / corr_one) / (jnp.sqrt(moment_two / corr_two) + ADAM_EPS)
    master = master - LEARN_RATE * (step_dir + WEIGHT_DECAY * master)
    return master, moment_one, moment_two


def forward_rows(x_rows, up_stack, down_stack):
    for layer_id in range(LAYERS):
        hidden = jnp.dot(x_rows, up_stack[layer_id], preferred_element_type=jnp.float32)
        gelu_out = jax.nn.gelu(hidden).astype(jnp.bfloat16)
        mlp_val = jnp.dot(gelu_out, down_stack[layer_id], preferred_element_type=jnp.float32)
        x_rows = (x_rows.astype(jnp.float32) + mlp_val).astype(jnp.bfloat16)
    return x_rows


def reference(x_saved, grad_out, x_next, w_up, w_down, acc_up, acc_down, master_up, master_down, moment1_up, moment1_down, moment2_up, moment2_down):
    grads_up = []
    grads_down = []
    for stage_id in range(STAGES):
        sum_up, sum_down = stage_grads(x_saved[stage_id], grad_out[stage_id], w_up[stage_id], w_down[stage_id])
        grads_up.append(sum_up)
        grads_down.append(sum_down)
    new_master_up, new_moment1_up, new_moment2_up = adam_update(acc_up, jnp.stack(grads_up), master_up, moment1_up, moment2_up)
    new_master_down, new_moment1_down, new_moment2_down = adam_update(acc_down, jnp.stack(grads_down), master_down, moment1_down, moment2_down)
    new_up = new_master_up.astype(jnp.bfloat16)
    new_down = new_master_down.astype(jnp.bfloat16)
    outs_next = []
    for stage_id in range(STAGES):
        row_blocks = x_next[stage_id].reshape(GROUPS, TOKENS, D)
        moved = lax.map(functools.partial(forward_rows, up_stack=new_up[stage_id], down_stack=new_down[stage_id]), row_blocks)
        outs_next.append(moved.reshape(BATCH, SEQ_LEN, D))
    y_next = jnp.stack(outs_next)
    return (new_master_up, new_master_down, new_moment1_up, new_moment1_down, new_moment2_up, new_moment2_down, y_next)
```

```python
import functools
import jax
import jax.numpy as jnp
from jax import lax
from jax.experimental import pallas as pl
from jax.experimental.pallas import tpu as pltpu
from jax.sharding import PartitionSpec as P

LEARN_RATE = 0.005
BETA_ONE = 0.9
BETA_TWO = 0.95
ADAM_EPS = 1e-8
WEIGHT_DECAY = 0.1
MICROBATCHES = 2
ADAM_STEP = 2
MESH = pl.DeviceIdType.MESH

ORDERS = ((2, 1, 0), (1, 0, 2), (0, 2, 1))
RS_LANES = ((0, 768), (768, 640), (1408, 640))
AG_LANES = ((0, 384), (384, 384), (768, 256))
TASKS = ((0, 1), (0, 0), (1, 1), (1, 0))
PHASES = 13
STAGGER = 2


def adam_update(acc_part, grad_new, master, moment_one, moment_two):
    grad_mean = (acc_part + grad_new) / MICROBATCHES
    moment_one = BETA_ONE * moment_one + (1.0 - BETA_ONE) * grad_mean
    moment_two = BETA_TWO * moment_two + (1.0 - BETA_TWO) * grad_mean * grad_mean
    corr_one = 1.0 - BETA_ONE ** ADAM_STEP
    corr_two = 1.0 - BETA_TWO ** ADAM_STEP
    step_dir = (moment_one / corr_one) / (jnp.sqrt(moment_two / corr_two) + ADAM_EPS)
    master = master - LEARN_RATE * (step_dir + WEIGHT_DECAY * master)
    return master, moment_one, moment_two


def backward_layer(x_in, cotangent, w_one, w_two):
    hidden = jnp.einsum('bsd,df->bsf', x_in, w_one, preferred_element_type=jnp.float32)
    gelu_out, gelu_vjp = jax.vjp(jax.nn.gelu, hidden)
    grad_act = jnp.einsum('bsd,fd->bsf', cotangent, w_two, preferred_element_type=jnp.float32)
    grad_hidden = gelu_vjp(grad_act)[0].astype(jnp.bfloat16)
    part_down = jnp.einsum('bsf,bsd->fd', gelu_out.astype(jnp.bfloat16), cotangent, preferred_element_type=jnp.float32)
    part_up = jnp.einsum('bsd,bsf->df', x_in, grad_hidden, preferred_element_type=jnp.float32)
    return part_up.astype(jnp.bfloat16), part_down.astype(jnp.bfloat16), grad_hidden


def forward_layer(x_in, w_one, w_two):
    hidden = jnp.einsum('bsd,df->bsf', x_in, w_one, preferred_element_type=jnp.float32)
    gelu_out = jax.nn.gelu(hidden).astype(jnp.bfloat16)
    mlp_val = jnp.einsum('bsf,fd->bsd', gelu_out, w_two, preferred_element_type=jnp.float32)
    return (x_in.astype(jnp.float32) + mlp_val).astype(jnp.bfloat16)


def half_dim(axis):
    return 1 if axis == 0 else 0


def region(fixed, lanes):
    return tuple(fixed.get(dim, slice(None)) for dim in range(3)) + (slice(None), pl.ds(lanes[0], lanes[1]))


def comm_kernel(*refs):
    ups, downs = refs[0:4], refs[4:8]
    acc_up, acc_down, master_up, master_down, m1_up, m1_down, m2_up, m2_down = refs[8:16]
    out_states = refs[16:22]
    gath_out = refs[22]
    (own_up, own_down, recv_up, recv_down, plane, rs1, rs2, rs3, rs4, grad_x, part_x, block8, gath, local_sem, send_sem, recv_sem) = refs[23:]

    me = lax.axis_index('fsdp')
    core = lax.rem(me, 2)
    chip = lax.div(me, 2)
    pos = (lax.div(chip, 16), lax.rem(lax.div(chip, 4), 4), lax.rem(chip, 4))
    stride = (32, 8, 2)
    partner = me + 1 - 2 * core

    def at_axis(axis, step):
        return lax.rem(pos[axis] + step, 4)

    def peer(axis, step):
        return me + (at_axis(axis, step) - pos[axis]) * stride[axis]

    barrier = pltpu.get_barrier_semaphore()
    pl.semaphore_signal(barrier, inc=1, device_id=(partner,), device_id_type=MESH)
    for axis in range(3):
        for step in (1, 2, 3):
            pl.semaphore_signal(barrier, inc=1, device_id=(peer(axis, step),), device_id_type=MESH)
    pl.semaphore_wait(barrier, 10)

    class Task:
        def __init__(self, task_id):
            self.t = task_id
            self.par = task_id % 2
            self.slot = 0
            self.live = []
            self.stage, self.layer = TASKS[task_id]

        def send(self, src, dst, device):
            copy = pltpu.make_async_remote_copy(src_ref=src, dst_ref=dst, send_sem=send_sem.at[self.t, self.slot], recv_sem=recv_sem.at[self.t, self.slot], device_id=(device,), device_id_type=MESH)
            self.slot += 1
            copy.start()
            self.live.append(copy)

        def drain(self):
            for copy in self.live:
                copy.wait()
            self.live = []

        def plane_at(self, fixed, g):
            return plane.at[(self.par,) + region(fixed, RS_LANES[g])]

        def gath_at(self, fixed, g):
            return gath.at[(self.t, core) + region(fixed, AG_LANES[g])]

        def run(self, phase):
            getattr(self, 'phase_%d' % phase)()

        def phase_0(self):
            t, par = self.t, self.par
            self.send(ups[t].at[:, pl.ds(pl.multiple_of((1 - core) * 1024, 1024), 1024)], recv_up.at[t], partner)
            self.send(downs[t].at[:, 1 - core], recv_down.at[t], partner)
            first = pltpu.make_async_copy(ups[t].at[:, pl.ds(pl.multiple_of(core * 1024, 1024), 1024)], own_up.at[par], local_sem.at[t, 0])
            second = pltpu.make_async_copy(downs[t].at[:, core], own_down.at[par], local_sem.at[t, 1])
            first.start()
            second.start()
            self.local = [first, second]

        def phase_1(self):
            t, par = self.t, self.par
            for copy in self.local:
                copy.wait()
            self.drain()

            def body(i, carry):
                z_pos, y_pos = lax.div(i, 4), lax.rem(i, 4)
                rows = pl.ds(pl.multiple_of(i * 32, 32), 32)
                up_sum = own_up[par, rows, :].astype(jnp.float32) + recv_up[t, rows, :].astype(jnp.float32)
                plane[par, z_pos, y_pos, :, :, 0:1024] = up_sum.reshape(4, 8, 1024)
                chips = pl.ds(i * 4, 4)
                down_sum = own_down[par, chips].astype(jnp.float32) + recv_down[t, chips].astype(jnp.float32)
                plane[par, z_pos, y_pos, :, :, 1024:1536] = down_sum[:, 0:8, :]
                plane[par, z_pos, y_pos, :, :, 1536:2048] = down_sum[:, 8:16, :]
                return carry

            lax.fori_loop(0, 16, body, 0)
            for g, order in enumerate(ORDERS):
                axis, half = order[0], half_dim(order[0])
                lanes = pl.ds(*RS_LANES[g])
                far = at_axis(axis, 2)
                self.send(self.plane_at({axis: far, half: pl.ds(0, 2)}, g), rs1.at[t, 0, :, :, :, lanes], peer(axis, 1))
                self.send(self.plane_at({axis: far, half: pl.ds(2, 2)}, g), rs1.at[t, 1, :, :, :, lanes], peer(axis, 3))

        def phase_2(self):
            t, par = self.t, self.par
            self.drain()
            for g, order in enumerate(ORDERS):
                axis, half = order[0], half_dim(order[0])
                lanes = pl.ds(*RS_LANES[g])
                for way, step in ((0, 1), (1, 3)):
                    dest = at_axis(axis, step)
                    where = (par,) + region({axis: dest, half: pl.ds(2 * way, 2)}, RS_LANES[g])
                    plane[where] = plane[where] + rs1[t, way, :, :, :, lanes]
                    self.send(self.plane_at({axis: dest}, g), rs2.at[t, way, :, :, :, lanes], peer(axis, step))

        def phase_3(self):
            t, par = self.t, self.par
            self.drain()
            for g, order in enumerate(ORDERS):
                lanes = pl.ds(*RS_LANES[g])
                where = (par,) + region({order[0]: pos[order[0]]}, RS_LANES[g])
                plane[where] = plane[where] + (rs2[t, 0, :, :, :, lanes] + rs2[t, 1, :, :, :, lanes])
                for step in (1, 2, 3):
                    self.send(self.plane_at({order[0]: pos[order[0]], order[1]: at_axis(order[1], step)}, g), rs3.at[t, step - 1, :, :, lanes], peer(order[1], step))

        def phase_4(self):
            t, par = self.t, self.par
            self.drain()
            for g, order in enumerate(ORDERS):
                lanes = pl.ds(*RS_LANES[g])
                fixed = {order[0]: pos[order[0]], order[1]: pos[order[1]]}
                where = (par,) + region(fixed, RS_LANES[g])
                plane[where] = plane[where] + (rs3[t, 0, :, :, lanes] + rs3[t, 1, :, :, lanes] + rs3[t, 2, :, :, lanes])
                for step in (1, 2, 3):
                    self.send(self.plane_at({**fixed, order[2]: at_axis(order[2], step)}, g), rs4.at[t, step - 1, :, lanes], peer(order[2], step))

        def phase_5(self):
            t, par = self.t, self.par
            self.drain()
            block = plane[par, pos[0], pos[1], pos[2]] + (rs4[t, 0] + rs4[t, 1] + rs4[t, 2])
            block8[t] = block
            grad_x[t, core] = block[:, 0:1024]
            self.send(grad_x.at[t, core], grad_x.at[t, core], partner)

        def phase_6(self):
            t, s, l = self.t, self.stage, self.layer
            self.drain()
            grad_down = jnp.concatenate([block8[t, :, 1024:1536], block8[t, :, 1536:2048]], axis=0)
            new_down = adam_update(acc_down[s, l], grad_down, master_down[s, l], m1_down[s, l], m2_down[s, l])
            low = jnp.concatenate([grad_x[t, 0, 0:4, :], grad_x[t, 1, 0:4, :]], axis=1)
            high = jnp.concatenate([grad_x[t, 0, 4:8, :], grad_x[t, 1, 4:8, :]], axis=1)
            grad_up = jnp.where(core == 0, low, high)
            new_up = adam_update(acc_up[s, l], grad_up, master_up[s, l], m1_up[s, l], m2_up[s, l])
            for i in range(3):
                out_states[2 * i][s, l] = new_up[i]
                out_states[2 * i + 1][s, l] = new_down[i]
            left, right = new_up[0][:, 0:1024], new_up[0][:, 1024:2048]
            part_x[t, core] = jnp.where(core == 0, left, right)
            part_x[t, 2] = jnp.where(core == 0, right, left)
            self.send(part_x.at[t, 2], part_x.at[t, core], partner)
            gath[t, core, pos[0], pos[1], pos[2], :, 512:1024] = new_down[0].astype(jnp.bfloat16)

        def phase_7(self):
            t = self.t
            self.drain()
            block8[t, 0:4, 0:1024] = part_x[t, 0]
            block8[t, 4:8, 0:1024] = part_x[t, 1]
            rows = jnp.concatenate([block8[t, :, 0:512], block8[t, :, 512:1024]], axis=0)
            gath[t, core, pos[0], pos[1], pos[2], :, 0:512] = rows.astype(jnp.bfloat16)
            for g, order in enumerate(ORDERS):
                where = self.gath_at({0: pos[0], 1: pos[1], 2: pos[2]}, g)
                for step in (1, 2, 3):
                    self.send(where, where, peer(order[2], step))

        def phase_8(self):
            self.drain()
            for g, order in enumerate(ORDERS):
                where = self.gath_at({order[0]: pos[order[0]], order[1]: pos[order[1]]}, g)
                for step in (1, 2, 3):
                    self.send(where, where, peer(order[1], step))

        def phase_9(self):
            self.drain()
            for g, order in enumerate(ORDERS):
                where = self.gath_at({order[0]: pos[order[0]]}, g)
                for step in (1, 3):
                    self.send(where, where, peer(order[0], step))

        def phase_10(self):
            self.drain()
            for g, order in enumerate(ORDERS):
                axis, half = order[0], half_dim(order[0])
                for way, step in ((0, 1), (1, 3)):
                    where = self.gath_at({axis: at_axis(axis, 4 - step), half: pl.ds(2 * way, 2)}, g)
                    self.send(where, where, peer(axis, step))

        def phase_11(self):
            self.drain()
            self.send(gath.at[self.t, core], gath.at[self.t, core], partner)

        def phase_12(self):
            self.drain()
            copy = pltpu.make_async_copy(gath.at[self.t], gath_out.at[self.t], local_sem.at[self.t, 2])
            copy.start()
            self.local = [copy]

    tasks = [Task(t) for t in range(4)]
    for tick in range(PHASES + 3 * STAGGER):
        for t in range(4):
            phase = tick - STAGGER * t
            if 0 <= phase < PHASES:
                tasks[t].run(phase)
    for task in tasks:
        for copy in task.local:
            copy.wait()


def communicate(ups, downs, states):
    vmem = pl.BlockSpec(memory_space=pltpu.VMEM)
    hbm = pl.BlockSpec(memory_space=pl.ANY)
    up_state = jax.ShapeDtypeStruct(states[0].shape, jnp.float32)
    down_state = jax.ShapeDtypeStruct(states[1].shape, jnp.float32)
    scratch = [
        pltpu.VMEM((2, 512, 1024), jnp.bfloat16),
        pltpu.VMEM((2, 64, 16, 512), jnp.bfloat16),
        pltpu.VMEM((4, 512, 1024), jnp.bfloat16),
        pltpu.VMEM((4, 64, 16, 512), jnp.bfloat16),
        pltpu.VMEM((2, 4, 4, 4, 8, 2048), jnp.float32),
        pltpu.VMEM((4, 2, 2, 4, 8, 2048), jnp.float32),
        pltpu.VMEM((4, 2, 4, 4, 8, 2048), jnp.float32),
        pltpu.VMEM((4, 3, 4, 8, 2048), jnp.float32),
        pltpu.VMEM((4, 3, 8, 2048), jnp.float32),
        pltpu.VMEM((4, 2, 8, 1024), jnp.float32),
        pltpu.VMEM((4, 3, 4, 1024), jnp.float32),
        pltpu.VMEM((4, 8, 2048), jnp.float32),
        pltpu.VMEM((4, 2, 4, 4, 4, 16, 1024), jnp.bfloat16),
        pltpu.SemaphoreType.DMA((4, 3)),
        pltpu.SemaphoreType.DMA((4, 66)),
        pltpu.SemaphoreType.DMA((4, 66)),
    ]
    return pl.pallas_call(
        comm_kernel,
        out_shape=(up_state, down_state) * 3 + (jax.ShapeDtypeStruct((4, 2, 4, 4, 4, 16, 1024), jnp.bfloat16),),
        in_specs=[hbm] * 8 + [vmem] * 8,
        out_specs=(vmem,) * 6 + (hbm,),
        scratch_shapes=scratch,
        compiler_params=pltpu.CompilerParams(collective_id=0, has_side_effects=True, vmem_limit_bytes=67043328),
        name='exchange',
    )(*ups, *downs, *states)


def solution(mesh):
    tok_spec = P(None, 'fsdp')
    layer_spec = P(None, None, 'fsdp')
    rep_spec = P()

    def device_step(x_saved, grad_out, x_next, w_up, w_down, acc_up, acc_down, master_up, master_down, moment1_up, moment1_down, moment2_up, moment2_down):
        ups, downs = [], []
        for stage_id in range(2):
            cotangent = grad_out[stage_id]
            for layer_id in (1, 0):
                cur_up = w_up[stage_id, layer_id]
                part_up, part_down, grad_hidden = backward_layer(x_saved[stage_id, layer_id], cotangent, cur_up, w_down[stage_id, layer_id])
                if layer_id > 0:
                    cotangent = (cotangent.astype(jnp.float32) + jnp.einsum('bsf,df->bsd', grad_hidden, cur_up, preferred_element_type=jnp.float32)).astype(jnp.bfloat16)
                ups.append(part_up)
                downs.append(part_down.reshape(64, 2, 16, 512))
        result = communicate(ups, downs, (acc_up, acc_down, master_up, master_down, moment1_up, moment1_down, moment2_up, moment2_down))
        gath = result[6].reshape(4, 2, 64, 16, 1024)
        y_list = []
        for stage_id in range(2):
            hidden_x = x_next[stage_id]
            for layer_id in range(2):
                part = gath[TASKS.index((stage_id, layer_id))]
                full_down = part[:, :, :, 512:].transpose(1, 0, 2, 3).reshape(2048, 512)
                full_up = part[:, :, :, :512].reshape(2, 64, 2, 8, 512).transpose(1, 3, 0, 2, 4).reshape(512, 2048)
                hidden_x = forward_layer(hidden_x, full_up, full_down)
            y_list.append(hidden_x)
        return result[:6] + (jnp.stack(y_list),)

    return jax.shard_map(device_step, mesh=mesh, in_specs=(layer_spec, tok_spec, tok_spec, rep_spec, rep_spec) + (layer_spec,) * 8, out_specs=(layer_spec,) * 6 + (tok_spec,), check_vma=False)
```

```python
import jax
import jax.numpy as jnp
from jax import lax
from jax.experimental import pallas as pl
from jax.experimental.pallas import tpu as pltpu
from jax.sharding import PartitionSpec as P

LEARN_RATE = 0.005
BETA_ONE = 0.9
BETA_TWO = 0.95
ADAM_EPS = 1e-8
WEIGHT_DECAY = 0.1
MICROBATCHES = 2
ADAM_STEP = 2
MESH = pl.DeviceIdType.MESH

ORDERS = ((2, 1, 0), (1, 0, 2), (0, 2, 1))
RS_LANES = ((0, 768), (768, 640), (1408, 640))
AG_LANES = ((0, 384), (384, 384), (768, 256))
TASKS = ((0, 1), (0, 0), (1, 1), (1, 0))
TILES = 8
RING = 4
SUB = 8
ROWS = 16
DIM = 512
HALF = 1024
FF = 2048
WIDTH = 256
OFFSETS = (0, 2, 6, 13, 17, 20, 21, 22, 24, 27, 32, 35, 39)
FORWARD = ((1, 0, 0), (0, 0, 1), (3, 1, 0), (2, 1, 1))
GELU_A = 0.7978845608028654
GELU_B = GELU_A * 0.044715


def adam_update(acc_part, grad_new, master, moment_one, moment_two):
    grad_mean = (acc_part + grad_new) / MICROBATCHES
    moment_one = BETA_ONE * moment_one + (1.0 - BETA_ONE) * grad_mean
    moment_two = BETA_TWO * moment_two + (1.0 - BETA_TWO) * grad_mean * grad_mean
    corr_one = 1.0 - BETA_ONE ** ADAM_STEP
    corr_two = 1.0 - BETA_TWO ** ADAM_STEP
    step_dir = (moment_one / corr_one) / (jnp.sqrt(moment_two / corr_two) + ADAM_EPS)
    master = master - LEARN_RATE * (step_dir + WEIGHT_DECAY * master)
    return master, moment_one, moment_two


def mm(a, b, a_dim, b_dim):
    return lax.dot_general(a, b, (((a_dim,), (b_dim,)), ((), ())), preferred_element_type=jnp.float32)


def half_dim(axis):
    return 1 if axis == 0 else 0


def region(fixed, lanes):
    return tuple(fixed.get(dim, slice(None)) for dim in range(3)) + (slice(None), pl.ds(lanes[0], lanes[1]))


def step_kernel(*refs):
    x_saved, grad_out, x_next, w_up, w_down = refs[0:5]
    acc_up, acc_down, master_up, master_down, m1_up, m1_down, m2_up, m2_down = refs[5:13]
    out_states = refs[13:19]
    y_out = refs[19]
    (wu, wd, xbuf, cot, total, plane, rs1, rs2, rs3, rs4, grad_x, part_x, block8, gath, w_sem, x_sem, send_sem, recv_sem, free_sem) = refs[20:]

    me = lax.axis_index('fsdp')
    core = lax.rem(me, 2)
    chip = lax.div(me, 2)
    pos = (lax.div(chip, ROWS), lax.rem(lax.div(chip, RING), RING), lax.rem(chip, RING))
    stride = (32, SUB, 2)
    partner = me + 1 - 2 * core
    near = [[lax.rem(pos[axis] + step, RING) for step in range(RING)] for axis in range(3)]
    peers = [[me + (near[axis][step] - pos[axis]) * stride[axis] for step in range(RING)] for axis in range(3)]

    def tile_of(i):
        return lax.rem(i + RING * (1 - core), TILES)

    def weight_copies(t, i):
        s, l = TASKS[t]
        cols = pl.ds(pl.multiple_of(tile_of(i) * WIDTH, WIDTH), WIDTH)
        return (pltpu.make_async_copy(w_up.at[s, l, :, cols], wu.at[i], w_sem.at[0, i]),
                pltpu.make_async_copy(w_down.at[s, l, cols, :], wd.at[i], w_sem.at[1, i]))

    def x_copy(t):
        s, l = TASKS[t]
        return pltpu.make_async_copy(x_saved.at[s, l, 0], xbuf.at[t % 2], x_sem.at[t % 2])

    def next_copy(s):
        return pltpu.make_async_copy(x_next.at[s, 0], xbuf.at[s], x_sem.at[s])

    def cot_copy(s):
        return pltpu.make_async_copy(grad_out.at[s, 0], cot.at[s], x_sem.at[2 + s])

    def y_copy(s):
        return pltpu.make_async_copy(xbuf.at[s], y_out.at[s, 0], x_sem.at[RING + s])

    x_copy(0).start()
    cot_copy(0).start()

    def first_weights(i, carry):
        for copy in weight_copies(0, i):
            copy.start()
        return carry

    lax.fori_loop(0, TILES, first_weights, 0)
    x_copy(1).start()
    cot_copy(1).start()

    barrier = pltpu.get_barrier_semaphore()
    pl.semaphore_signal(barrier, inc=1, device_id=(partner,), device_id_type=MESH)
    for axis in range(3):
        for step in (1, 2, 3):
            pl.semaphore_signal(barrier, inc=1, device_id=(peers[axis][step],), device_id_type=MESH)
    pl.semaphore_wait(barrier, 10)

    class Task:
        def __init__(self, task_id):
            self.t = task_id
            self.par = task_id % 2
            self.slot = 0
            self.live = []
            self.stage, self.layer = TASKS[task_id]

        def send(self, src, dst, device):
            slot = self.slot
            self.slot += 1

            def make():
                return pltpu.make_async_remote_copy(src_ref=src(), dst_ref=dst(), send_sem=send_sem.at[self.t, slot], recv_sem=recv_sem.at[self.t, slot], device_id=(device,), device_id_type=MESH)

            make().start()
            self.live.append(make)

        def drain(self):
            for make in self.live:
                make().wait()
            self.live = []

        def plane_at(self, fixed, g):
            return lambda: plane.at[(self.t,) + region(fixed, RS_LANES[g])]

        def gath_at(self, fixed, g):
            return lambda: gath.at[(self.t, core) + region(fixed, AG_LANES[g])]

        def run(self, phase):
            getattr(self, 'phase_%s' % phase)()

        def phase_up(self):
            self.send(lambda: gath.at[self.t, 1, 0:2], lambda: gath.at[self.t, 0, 0:2], partner)

        def phase_0(self):
            self.send(lambda: gath.at[self.t, 1, 2:RING], lambda: gath.at[self.t, 0, 2:RING], partner)

        def phase_1(self):
            t, par = self.t, self.par
            self.drain()

            def body(i, carry):
                z_pos, y_pos = lax.div(i, RING), lax.rem(i, RING)
                z_blk, y_blk, x_blk = lax.div(i, SUB), lax.div(lax.rem(i, SUB), 2), 2 * lax.rem(i, 2)
                up_part = gath[t, 0, z_blk, y_blk, pl.ds(x_blk, 2)].astype(jnp.float32)
                plane[t, z_pos, y_pos, :, :, 0:HALF] = plane[t, z_pos, y_pos, :, :, 0:HALF] + up_part.reshape(RING, SUB, HALF)
                down_part = gath[t, 0, z_blk + 2, y_blk, pl.ds(x_blk, 2)].astype(jnp.float32)
                for k in range(2):
                    for m in range(2):
                        for h in range(2):
                            lanes = slice(HALF + DIM * h, HALF + DIM * (h + 1))
                            plane[t, z_pos, y_pos, 2 * k + m, :, lanes] = plane[t, z_pos, y_pos, 2 * k + m, :, lanes] + down_part[k, SUB * h:SUB * h + SUB, DIM * m:DIM * m + DIM]
                return carry

            lax.fori_loop(0, ROWS, body, 0)
            for g, order in enumerate(ORDERS):
                axis, half = order[0], half_dim(order[0])
                lanes = pl.ds(*RS_LANES[g])
                for way, step in ((0, 1), (1, 3)):
                    self.send(self.plane_at({axis: near[axis][2], half: pl.ds(2 * way, 2)}, g), lambda way=way, lanes=lanes: rs1.at[par, way, :, :, :, lanes], peers[axis][step])

        def phase_2(self):
            t, par = self.t, self.par
            self.drain()
            for g, order in enumerate(ORDERS):
                axis, half = order[0], half_dim(order[0])
                lanes = pl.ds(*RS_LANES[g])
                for way, step in ((0, 1), (1, 3)):
                    where = (t,) + region({axis: near[axis][step], half: pl.ds(2 * way, 2)}, RS_LANES[g])
                    plane[where] = plane[where] + rs1[par, way, :, :, :, lanes]
            for g, order in enumerate(ORDERS):
                axis = order[0]
                lanes = pl.ds(*RS_LANES[g])
                for way, step in ((0, 1), (1, 3)):
                    if t >= 2:
                        pl.semaphore_wait(free_sem.at[0, par, g, way], 1)
                    self.send(self.plane_at({axis: near[axis][step]}, g), lambda way=way, lanes=lanes: rs2.at[par, way, :, :, :, lanes], peers[axis][step])

        def phase_3(self):
            t, par = self.t, self.par
            self.drain()
            for g, order in enumerate(ORDERS):
                lanes = pl.ds(*RS_LANES[g])
                where = (t,) + region({order[0]: pos[order[0]]}, RS_LANES[g])
                plane[where] = plane[where] + (rs2[par, 0, :, :, :, lanes] + rs2[par, 1, :, :, :, lanes])
                if t < 2:
                    for way, step in ((0, 3), (1, 1)):
                        pl.semaphore_signal(free_sem.at[0, par, g, way], inc=1, device_id=(peers[order[0]][step],), device_id_type=MESH)
            for g, order in enumerate(ORDERS):
                lanes = pl.ds(*RS_LANES[g])
                axis = order[1]
                for step in (1, 2, 3):
                    if t >= 2:
                        pl.semaphore_wait(free_sem.at[1, par, g, step - 1], 1)
                    self.send(self.plane_at({order[0]: pos[order[0]], axis: near[axis][step]}, g), lambda step=step, lanes=lanes: rs3.at[par, step - 1, :, :, lanes], peers[axis][step])

        def phase_4(self):
            t, par = self.t, self.par
            self.drain()
            for g, order in enumerate(ORDERS):
                lanes = pl.ds(*RS_LANES[g])
                where = (t,) + region({order[0]: pos[order[0]], order[1]: pos[order[1]]}, RS_LANES[g])
                plane[where] = plane[where] + (rs3[par, 0, :, :, lanes] + rs3[par, 1, :, :, lanes] + rs3[par, 2, :, :, lanes])
                if t < 2:
                    for step in (1, 2, 3):
                        pl.semaphore_signal(free_sem.at[1, par, g, step - 1], inc=1, device_id=(peers[order[1]][RING - step],), device_id_type=MESH)
            for g, order in enumerate(ORDERS):
                lanes = pl.ds(*RS_LANES[g])
                axis = order[2]
                fixed = {order[0]: pos[order[0]], order[1]: pos[order[1]]}
                for step in (1, 2, 3):
                    self.send(self.plane_at({**fixed, axis: near[axis][step]}, g), lambda step=step, lanes=lanes: rs4.at[t, step - 1, :, lanes], peers[axis][step])

        def phase_5(self):
            t = self.t
            self.drain()
            block = plane[t, pos[0], pos[1], pos[2]] + (rs4[t, 0] + rs4[t, 1] + rs4[t, 2])
            block8[t] = block
            grad_x[t, core] = block[:, 0:HALF]
            self.send(lambda: grad_x.at[t, core], lambda: grad_x.at[t, core], partner)

        def phase_6(self):
            t, s, l = self.t, self.stage, self.layer
            self.drain()
            grad_down = jnp.concatenate([block8[t, :, HALF:HALF + DIM], block8[t, :, HALF + DIM:FF]], axis=0)
            new_down = adam_update(acc_down[s, l], grad_down, master_down[s, l], m1_down[s, l], m2_down[s, l])
            low = jnp.concatenate([grad_x[t, 0, 0:RING, :], grad_x[t, 1, 0:RING, :]], axis=1)
            high = jnp.concatenate([grad_x[t, 0, RING:SUB, :], grad_x[t, 1, RING:SUB, :]], axis=1)
            grad_up = jnp.where(core == 0, low, high)
            new_up = adam_update(acc_up[s, l], grad_up, master_up[s, l], m1_up[s, l], m2_up[s, l])
            for i in range(3):
                out_states[2 * i][s, l] = new_up[i]
                out_states[2 * i + 1][s, l] = new_down[i]
            left, right = new_up[0][:, 0:HALF], new_up[0][:, HALF:FF]
            part_x[t, core] = jnp.where(core == 0, left, right)
            part_x[t, 2] = jnp.where(core == 0, right, left)
            self.send(lambda: part_x.at[t, 2], lambda: part_x.at[t, core], partner)
            gath[t, core, pos[0], pos[1], pos[2], :, DIM:HALF] = new_down[0].astype(jnp.bfloat16)

        def phase_7(self):
            t = self.t
            self.drain()
            block8[t, 0:RING, 0:HALF] = part_x[t, 0]
            block8[t, RING:SUB, 0:HALF] = part_x[t, 1]
            rows = jnp.concatenate([block8[t, :, 0:DIM], block8[t, :, DIM:HALF]], axis=0)
            gath[t, core, pos[0], pos[1], pos[2], :, 0:DIM] = rows.astype(jnp.bfloat16)
            for g, order in enumerate(ORDERS):
                where = self.gath_at({0: pos[0], 1: pos[1], 2: pos[2]}, g)
                for step in (1, 2, 3):
                    self.send(where, where, peers[order[2]][step])

        def phase_8(self):
            self.drain()
            for g, order in enumerate(ORDERS):
                where = self.gath_at({order[0]: pos[order[0]], order[1]: pos[order[1]]}, g)
                for step in (1, 2, 3):
                    self.send(where, where, peers[order[1]][step])

        def phase_9(self):
            self.drain()
            for g, order in enumerate(ORDERS):
                where = self.gath_at({order[0]: pos[order[0]]}, g)
                for step in (1, 3):
                    self.send(where, where, peers[order[0]][step])

        def phase_10(self):
            self.drain()
            for g, order in enumerate(ORDERS):
                axis, half = order[0], half_dim(order[0])
                for way, step in ((0, 1), (1, 3)):
                    where = self.gath_at({axis: near[axis][RING - step], half: pl.ds(2 * way, 2)}, g)
                    self.send(where, where, peers[axis][step])

        def phase_11(self):
            self.drain()
            self.send(lambda: gath.at[self.t, core], lambda: gath.at[self.t, core], partner)

        def phase_12(self):
            self.drain()

    tasks = [Task(t) for t in range(RING)]
    agenda = sorted((TILES * (t + 1) - 1 + offset, t, phase) for t in range(RING) for phase, offset in enumerate(OFFSETS))
    finished = set()

    def advance(now):
        while agenda and agenda[0][0] <= now:
            _, t, phase = agenda.pop(0)
            tasks[t].run(phase)
            finished.add((t, phase))

    def backward(t):
        s, l = TASKS[t]
        slot = t % 2
        x_copy(t).wait()
        if l == 1:
            cot_copy(s).wait()
            total[...] = jnp.zeros_like(total)

        def body(i, carry):
            j = tile_of(i)
            for copy in weight_copies(t, i):
                copy.wait()
            x, dy, w1, w2 = xbuf[slot], cot[s], wu[i], wd[i]
            h = mm(x, w1, 1, 0)
            grad_act = mm(dy, w2, 1, 1)
            square = h * h
            tanh = jnp.tanh(h * (GELU_A + GELU_B * square))
            gate = 0.5 * tanh + 0.5
            act = (h * gate).astype(jnp.bfloat16)
            slope = gate + (0.5 * h) * (1.0 - tanh * tanh) * (GELU_A + 3.0 * GELU_B * square)
            grad_h = (grad_act * slope).astype(jnp.bfloat16)
            down = mm(act, dy, 0, 0).reshape(SUB, 2, ROWS, DIM)
            own = jnp.where(core == 0, down[:, 0], down[:, 1])
            other = jnp.where(core == 0, down[:, 1], down[:, 0]).astype(jnp.bfloat16)
            rows = pl.ds(2 * lax.rem(j, 2), 2)
            plane[t, lax.div(j, 2), rows, :, :, HALF:HALF + DIM] = own[:, 0:SUB].reshape(2, RING, SUB, DIM)
            plane[t, lax.div(j, 2), rows, :, :, HALF + DIM:FF] = own[:, SUB:ROWS].reshape(2, RING, SUB, DIM)
            for k in range(RING):
                gath[t, 1, 2 + lax.div(j, RING), lax.rem(j, RING), k, :, 0:DIM] = other[2 * k]
                gath[t, 1, 2 + lax.div(j, RING), lax.rem(j, RING), k, :, DIM:HALF] = other[2 * k + 1]
            up = mm(x, grad_h, 0, 0)
            cols = pl.ds(pl.multiple_of(lax.rem(j, RING) * WIDTH, WIDTH), WIDTH)

            @pl.when(i < RING)
            def _():
                gath[t, 1, 0:2, :, :, :, cols] = up.astype(jnp.bfloat16).reshape(2, RING, RING, ROWS, WIDTH)

            @pl.when(i >= RING)
            def _():
                plane[t, :, :, :, :, cols] = up.reshape(RING, RING, RING, SUB, WIDTH)

            if l == 1:
                total[...] = total[...] + mm(grad_h, w1, 1, 1)
            if t < 3:
                for copy in weight_copies(t + 1, i):
                    copy.start()

            for k in range(TILES):
                if k == 3 or agenda and agenda[0][0] <= TILES * t + k:
                    @pl.when(i == k)
                    def _():
                        if k == 3:
                            tasks[t].run('up')
                        advance(TILES * t + k)
            return carry

        lax.fori_loop(0, TILES, body, 0)
        if l == 1:
            cot[s] = (cot[s].astype(jnp.float32) + total[...]).astype(jnp.bfloat16)
        if t < 2:
            x_copy(t + 2).start()
        else:
            next_copy(t - 2).start()

    def forward(t, s, l, now):
        if l == 0:
            next_copy(s).wait()
        total[...] = jnp.zeros_like(total)

        def body(i, carry):
            half, q, lane = lax.div(i, RING), lax.div(lax.rem(i, RING), 2), lax.rem(i, 2)
            lanes = pl.ds(pl.multiple_of(lane * WIDTH, WIDTH), WIDTH)
            raw = gath[t, half, :, :, :, :, lanes].astype(jnp.float32).reshape(64, ROWS, WIDTH)
            w1 = jnp.where(q == 0, raw[:, 0:SUB], raw[:, SUB:ROWS]).reshape(DIM, WIDTH).astype(jnp.bfloat16)
            rows = pl.ds(2 * lax.rem(i, 2), 2)
            even = gath[t, 0, lax.div(i, 2), rows, :, :, DIM:HALF].reshape(SUB, 1, ROWS, DIM)
            odd = gath[t, 1, lax.div(i, 2), rows, :, :, DIM:HALF].reshape(SUB, 1, ROWS, DIM)
            w2 = jnp.concatenate([even, odd], axis=1).reshape(WIDTH, DIM)
            h = mm(xbuf[s], w1, 1, 0)
            tanh = jnp.tanh(h * (GELU_A + GELU_B * (h * h)))
            act = (h * (0.5 * tanh + 0.5)).astype(jnp.bfloat16)
            total[...] = total[...] + mm(act, w2, 1, 0)
            for k in range(1, TILES, 2):
                if agenda and agenda[0][0] <= now + k // 2:
                    @pl.when(i == k)
                    def _():
                        advance(now + k // 2)
            return carry

        lax.fori_loop(0, TILES, body, 0)
        xbuf[s] = (xbuf[s].astype(jnp.float32) + total[...]).astype(jnp.bfloat16)
        if l == 1:
            y_copy(s).start()
        return now + TILES // 2

    for t in range(RING):
        backward(t)
    now = RING * TILES - 1
    for t, s, l in FORWARD:
        while (t, 12) not in finished:
            now = max(now, agenda[0][0])
            advance(agenda[0][0])
        now = forward(t, s, l, now)
    for s in range(2):
        y_copy(s).wait()


def fused_step(*args):
    vmem = pl.BlockSpec(memory_space=pltpu.VMEM)
    hbm = pl.BlockSpec(memory_space=pl.ANY)
    up_state = jax.ShapeDtypeStruct(args[5].shape, jnp.float32)
    down_state = jax.ShapeDtypeStruct(args[6].shape, jnp.float32)
    scratch = [
        pltpu.VMEM((TILES, DIM, WIDTH), jnp.bfloat16),
        pltpu.VMEM((TILES, WIDTH, DIM), jnp.bfloat16),
        pltpu.VMEM((2, HALF, DIM), jnp.bfloat16),
        pltpu.VMEM((2, HALF, DIM), jnp.bfloat16),
        pltpu.VMEM((HALF, DIM), jnp.float32),
        pltpu.VMEM((RING,) * RING + (SUB, FF), jnp.float32),
        pltpu.VMEM((2, 2, 2, RING, SUB, FF), jnp.float32),
        pltpu.VMEM((2, 2, RING, RING, SUB, FF), jnp.float32),
        pltpu.VMEM((2, 3, RING, SUB, FF), jnp.float32),
        pltpu.VMEM((RING, 3, SUB, FF), jnp.float32),
        pltpu.VMEM((RING, 2, SUB, HALF), jnp.float32),
        pltpu.VMEM((RING, 3, RING, HALF), jnp.float32),
        pltpu.VMEM((RING, SUB, FF), jnp.float32),
        pltpu.VMEM((RING, 2, RING, RING, RING, ROWS, HALF), jnp.bfloat16),
        pltpu.SemaphoreType.DMA((2, TILES)),
        pltpu.SemaphoreType.DMA((6,)),
        pltpu.SemaphoreType.DMA((RING, 66)),
        pltpu.SemaphoreType.DMA((RING, 66)),
        pltpu.SemaphoreType.REGULAR((2, 2, 3, 3)),
    ]
    return pl.pallas_call(
        step_kernel,
        out_shape=(up_state, down_state) * 3 + (jax.ShapeDtypeStruct(args[2].shape, jnp.bfloat16),),
        in_specs=[hbm] * 5 + [vmem] * SUB,
        out_specs=(vmem,) * 6 + (hbm,),
        scratch_shapes=scratch,
        compiler_params=pltpu.CompilerParams(collective_id=0, has_side_effects=True, vmem_limit_bytes=67043328),
        name='step',
    )(*args)


def solution(mesh):
    tok_spec = P(None, 'fsdp')
    layer_spec = P(None, None, 'fsdp')
    rep_spec = P()

    def device_step(*args):
        return tuple(fused_step(*args))

    return jax.shard_map(device_step, mesh=mesh, in_specs=(layer_spec, tok_spec, tok_spec, rep_spec, rep_spec) + (layer_spec,) * SUB, out_specs=(layer_spec,) * 6 + (tok_spec,), check_vma=False)
```

```python
import jax
import jax.numpy as jnp
from jax import lax
from jax.experimental import pallas as pl
from jax.experimental.pallas import tpu as pltpu
from jax.sharding import PartitionSpec as P

LEARN_RATE = 0.005
BETA_ONE = 0.9
BETA_TWO = 0.95
ADAM_EPS = 1e-8
WEIGHT_DECAY = 0.1
MICROBATCHES = 2
ADAM_STEP = 2
MESH = pl.DeviceIdType.MESH

ORDERS = ((2, 1, 0), (1, 0, 2), (0, 2, 1))
RS_LANES = ((0, 768), (768, 640), (1408, 640))
AG_LANES = ((0, 384), (384, 384), (768, 256))
TASKS = ((0, 1), (0, 0), (1, 1), (1, 0))
TILES = 8
CHUNK = 512
SPAN = 256
RING = 4
SUB = 8
ROWS = 16
DIM = 512
HALF = 1024
FF = 2048
WIDTH = 256
OFFSETS = (0, 2, 6, 13, 17, 20, 21, 22, 24, 27, 32, 35, 39)
FORWARD = ((1, 0, 0), (0, 0, 1), (3, 1, 0), (2, 1, 1))
GELU_A = 0.7978845608028654
GELU_B = GELU_A * 0.044715


def adam_update(acc_part, grad_new, master, moment_one, moment_two):
    grad_mean = (acc_part + grad_new) / MICROBATCHES
    moment_one = BETA_ONE * moment_one + (1.0 - BETA_ONE) * grad_mean
    moment_two = BETA_TWO * moment_two + (1.0 - BETA_TWO) * grad_mean * grad_mean
    corr_one = 1.0 - BETA_ONE ** ADAM_STEP
    corr_two = 1.0 - BETA_TWO ** ADAM_STEP
    step_dir = (moment_one / corr_one) / (jnp.sqrt(moment_two / corr_two) + ADAM_EPS)
    master = master - LEARN_RATE * (step_dir + WEIGHT_DECAY * master)
    return master, moment_one, moment_two


def mm(a, b, a_dim, b_dim):
    return lax.dot_general(a, b, (((a_dim,), (b_dim,)), ((), ())), preferred_element_type=jnp.float32)


def half_dim(axis):
    return 1 if axis == 0 else 0


def region(fixed, lanes):
    return tuple(fixed.get(dim, slice(None)) for dim in range(3)) + (slice(None), pl.ds(lanes[0], lanes[1]))


def step_kernel(*refs):
    x_saved, grad_out, x_next, w_up, w_down = refs[0:5]
    acc_up, acc_down, master_up, master_down, m1_up, m1_down, m2_up, m2_down = refs[5:13]
    out_states = refs[13:19]
    y_out = refs[19]
    (wu, wd, xbuf, cot, total, act_buf, grad_buf, plane, rs1, rs2, rs3, rs4, grad_x, part_x, block8, gath, w_sem, x_sem, send_sem, recv_sem, free_sem) = refs[20:]

    me = lax.axis_index('fsdp')
    core = lax.rem(me, 2)
    chip = lax.div(me, 2)
    pos = (lax.div(chip, ROWS), lax.rem(lax.div(chip, RING), RING), lax.rem(chip, RING))
    stride = (32, SUB, 2)
    partner = me + 1 - 2 * core
    near = [[lax.rem(pos[axis] + step, RING) for step in range(RING)] for axis in range(3)]
    peers = [[me + (near[axis][step] - pos[axis]) * stride[axis] for step in range(RING)] for axis in range(3)]

    def tile_of(i):
        return lax.rem(i + RING * (1 - core), TILES)

    def weight_copies(t, i):
        s, l = TASKS[t]
        cols = pl.ds(pl.multiple_of(tile_of(i) * WIDTH, WIDTH), WIDTH)
        return (pltpu.make_async_copy(w_up.at[s, l, :, cols], wu.at[i], w_sem.at[0, i]),
                pltpu.make_async_copy(w_down.at[s, l, cols, :], wd.at[i], w_sem.at[1, i]))

    def x_copy(t):
        s, l = TASKS[t]
        return pltpu.make_async_copy(x_saved.at[s, l, 0], xbuf.at[t % 2], x_sem.at[t % 2])

    def next_copy(s):
        return pltpu.make_async_copy(x_next.at[s, 0], xbuf.at[s], x_sem.at[s])

    def cot_copy(s):
        return pltpu.make_async_copy(grad_out.at[s, 0], cot.at[s], x_sem.at[2 + s])

    def y_copy(s):
        return pltpu.make_async_copy(xbuf.at[s], y_out.at[s, 0], x_sem.at[RING + s])

    x_copy(0).start()
    cot_copy(0).start()

    def first_weights(i, carry):
        for copy in weight_copies(0, i):
            copy.start()
        return carry

    lax.fori_loop(0, TILES, first_weights, 0)
    x_copy(1).start()
    cot_copy(1).start()

    barrier = pltpu.get_barrier_semaphore()
    pl.semaphore_signal(barrier, inc=1, device_id=(partner,), device_id_type=MESH)
    for axis in range(3):
        for step in (1, 2, 3):
            pl.semaphore_signal(barrier, inc=1, device_id=(peers[axis][step],), device_id_type=MESH)
    pl.semaphore_wait(barrier, 10)

    class Task:
        def __init__(self, task_id):
            self.t = task_id
            self.par = task_id % 2
            self.slot = 0
            self.live = []
            self.stage, self.layer = TASKS[task_id]

        def send(self, src, dst, device):
            slot = self.slot
            self.slot += 1

            def make():
                return pltpu.make_async_remote_copy(src_ref=src(), dst_ref=dst(), send_sem=send_sem.at[self.t, slot], recv_sem=recv_sem.at[self.t, slot], device_id=(device,), device_id_type=MESH)

            make().start()
            self.live.append(make)

        def drain(self):
            for make in self.live:
                make().wait()
            self.live = []

        def plane_at(self, fixed, g):
            return lambda: plane.at[(self.t,) + region(fixed, RS_LANES[g])]

        def gath_at(self, fixed, g):
            return lambda: gath.at[(self.t, core) + region(fixed, AG_LANES[g])]

        def run(self, phase):
            getattr(self, 'phase_%s' % phase)()

        def phase_up(self):
            self.send(lambda: gath.at[self.t, 1, 0:2], lambda: gath.at[self.t, 0, 0:2], partner)

        def phase_0(self):
            self.send(lambda: gath.at[self.t, 1, 2:RING], lambda: gath.at[self.t, 0, 2:RING], partner)

        def phase_1(self):
            t, par = self.t, self.par
            self.drain()

            def body(i, carry):
                z_pos, y_pos = lax.div(i, RING), lax.rem(i, RING)
                z_blk, y_blk, x_blk = lax.div(i, SUB), lax.div(lax.rem(i, SUB), 2), 2 * lax.rem(i, 2)
                up_part = gath[t, 0, z_blk, y_blk, pl.ds(x_blk, 2)].astype(jnp.float32)
                plane[t, z_pos, y_pos, :, :, 0:HALF] = plane[t, z_pos, y_pos, :, :, 0:HALF] + up_part.reshape(RING, SUB, HALF)
                down_part = gath[t, 0, z_blk + 2, y_blk, pl.ds(x_blk, 2)].astype(jnp.float32)
                for k in range(2):
                    for m in range(2):
                        for h in range(2):
                            lanes = slice(HALF + DIM * h, HALF + DIM * (h + 1))
                            plane[t, z_pos, y_pos, 2 * k + m, :, lanes] = plane[t, z_pos, y_pos, 2 * k + m, :, lanes] + down_part[k, SUB * h:SUB * h + SUB, DIM * m:DIM * m + DIM]
                return carry

            lax.fori_loop(0, ROWS, body, 0)
            for g, order in enumerate(ORDERS):
                axis, half = order[0], half_dim(order[0])
                lanes = pl.ds(*RS_LANES[g])
                for way, step in ((0, 1), (1, 3)):
                    self.send(self.plane_at({axis: near[axis][2], half: pl.ds(2 * way, 2)}, g), lambda way=way, lanes=lanes: rs1.at[par, way, :, :, :, lanes], peers[axis][step])

        def phase_2(self):
            t, par = self.t, self.par
            self.drain()
            for g, order in enumerate(ORDERS):
                axis, half = order[0], half_dim(order[0])
                lanes = pl.ds(*RS_LANES[g])
                for way, step in ((0, 1), (1, 3)):
                    where = (t,) + region({axis: near[axis][step], half: pl.ds(2 * way, 2)}, RS_LANES[g])
                    plane[where] = plane[where] + rs1[par, way, :, :, :, lanes]
            for g, order in enumerate(ORDERS):
                axis = order[0]
                lanes = pl.ds(*RS_LANES[g])
                for way, step in ((0, 1), (1, 3)):
                    if t >= 2:
                        pl.semaphore_wait(free_sem.at[0, par, g, way], 1)
                    self.send(self.plane_at({axis: near[axis][step]}, g), lambda way=way, lanes=lanes: rs2.at[par, way, :, :, :, lanes], peers[axis][step])

        def phase_3(self):
            t, par = self.t, self.par
            self.drain()
            for g, order in enumerate(ORDERS):
                lanes = pl.ds(*RS_LANES[g])
                where = (t,) + region({order[0]: pos[order[0]]}, RS_LANES[g])
                plane[where] = plane[where] + (rs2[par, 0, :, :, :, lanes] + rs2[par, 1, :, :, :, lanes])
                if t < 2:
                    for way, step in ((0, 3), (1, 1)):
                        pl.semaphore_signal(free_sem.at[0, par, g, way], inc=1, device_id=(peers[order[0]][step],), device_id_type=MESH)
            for g, order in enumerate(ORDERS):
                lanes = pl.ds(*RS_LANES[g])
                axis = order[1]
                for step in (1, 2, 3):
                    if t >= 2:
                        pl.semaphore_wait(free_sem.at[1, par, g, step - 1], 1)
                    self.send(self.plane_at({order[0]: pos[order[0]], axis: near[axis][step]}, g), lambda step=step, lanes=lanes: rs3.at[par, step - 1, :, :, lanes], peers[axis][step])

        def phase_4(self):
            t, par = self.t, self.par
            self.drain()
            for g, order in enumerate(ORDERS):
                lanes = pl.ds(*RS_LANES[g])
                where = (t,) + region({order[0]: pos[order[0]], order[1]: pos[order[1]]}, RS_LANES[g])
                plane[where] = plane[where] + (rs3[par, 0, :, :, lanes] + rs3[par, 1, :, :, lanes] + rs3[par, 2, :, :, lanes])
                if t < 2:
                    for step in (1, 2, 3):
                        pl.semaphore_signal(free_sem.at[1, par, g, step - 1], inc=1, device_id=(peers[order[1]][RING - step],), device_id_type=MESH)
            for g, order in enumerate(ORDERS):
                lanes = pl.ds(*RS_LANES[g])
                axis = order[2]
                fixed = {order[0]: pos[order[0]], order[1]: pos[order[1]]}
                for step in (1, 2, 3):
                    self.send(self.plane_at({**fixed, axis: near[axis][step]}, g), lambda step=step, lanes=lanes: rs4.at[t, step - 1, :, lanes], peers[axis][step])

        def phase_5(self):
            t = self.t
            self.drain()
            block = plane[t, pos[0], pos[1], pos[2]] + (rs4[t, 0] + rs4[t, 1] + rs4[t, 2])
            block8[t] = block
            grad_x[t, core] = block[:, 0:HALF]
            self.send(lambda: grad_x.at[t, core], lambda: grad_x.at[t, core], partner)

        def phase_6(self):
            t, s, l = self.t, self.stage, self.layer
            self.drain()
            grad_down = jnp.concatenate([block8[t, :, HALF:HALF + DIM], block8[t, :, HALF + DIM:FF]], axis=0)
            new_down = adam_update(acc_down[s, l], grad_down, master_down[s, l], m1_down[s, l], m2_down[s, l])
            low = jnp.concatenate([grad_x[t, 0, 0:RING, :], grad_x[t, 1, 0:RING, :]], axis=1)
            high = jnp.concatenate([grad_x[t, 0, RING:SUB, :], grad_x[t, 1, RING:SUB, :]], axis=1)
            grad_up = jnp.where(core == 0, low, high)
            new_up = adam_update(acc_up[s, l], grad_up, master_up[s, l], m1_up[s, l], m2_up[s, l])
            for i in range(3):
                out_states[2 * i][s, l] = new_up[i]
                out_states[2 * i + 1][s, l] = new_down[i]
            left, right = new_up[0][:, 0:HALF], new_up[0][:, HALF:FF]
            part_x[t, core] = jnp.where(core == 0, left, right)
            part_x[t, 2] = jnp.where(core == 0, right, left)
            self.send(lambda: part_x.at[t, 2], lambda: part_x.at[t, core], partner)
            gath[t, core, pos[0], pos[1], pos[2], :, DIM:HALF] = new_down[0].astype(jnp.bfloat16)

        def phase_7(self):
            t = self.t
            self.drain()
            block8[t, 0:RING, 0:HALF] = part_x[t, 0]
            block8[t, RING:SUB, 0:HALF] = part_x[t, 1]
            rows = jnp.concatenate([block8[t, :, 0:DIM], block8[t, :, DIM:HALF]], axis=0)
            gath[t, core, pos[0], pos[1], pos[2], :, 0:DIM] = rows.astype(jnp.bfloat16)
            for g, order in enumerate(ORDERS):
                where = self.gath_at({0: pos[0], 1: pos[1], 2: pos[2]}, g)
                for step in (1, 2, 3):
                    self.send(where, where, peers[order[2]][step])

        def phase_8(self):
            self.drain()
            for g, order in enumerate(ORDERS):
                where = self.gath_at({order[0]: pos[order[0]], order[1]: pos[order[1]]}, g)
                for step in (1, 2, 3):
                    self.send(where, where, peers[order[1]][step])

        def phase_9(self):
            self.drain()
            for g, order in enumerate(ORDERS):
                where = self.gath_at({order[0]: pos[order[0]]}, g)
                for step in (1, 3):
                    self.send(where, where, peers[order[0]][step])

        def phase_10(self):
            self.drain()
            for g, order in enumerate(ORDERS):
                axis, half = order[0], half_dim(order[0])
                for way, step in ((0, 1), (1, 3)):
                    where = self.gath_at({axis: near[axis][RING - step], half: pl.ds(2 * way, 2)}, g)
                    self.send(where, where, peers[axis][step])

        def phase_11(self):
            self.drain()
            self.send(lambda: gath.at[self.t, core], lambda: gath.at[self.t, core], partner)

        def phase_12(self):
            self.drain()

    tasks = [Task(t) for t in range(RING)]
    agenda = sorted((TILES * (t + 1) - 1 + offset, t, phase) for t in range(RING) for phase, offset in enumerate(OFFSETS))
    finished = set()

    def advance(now):
        while agenda and agenda[0][0] <= now:
            _, t, phase = agenda.pop(0)
            tasks[t].run(phase)
            finished.add((t, phase))

    def backward(t):
        s, l = TASKS[t]
        slot = t % 2
        x_copy(t).wait()
        if l == 1:
            cot_copy(s).wait()
            total[...] = jnp.zeros_like(total)

        def fetch(i):
            for copy in weight_copies(t, i):
                copy.wait()

        def front(i, m):
            rows = pl.ds(m * CHUNK, CHUNK)
            h = mm(xbuf[slot, rows, :], wu[i], 1, 0)
            grad_act = mm(cot[s, rows, :], wd[i], 1, 1)
            square = h * h
            tanh = jnp.tanh(h * (GELU_A + GELU_B * square))
            gate = 0.5 * tanh + 0.5
            act_buf[lax.rem(i, 2), rows, :] = (h * gate).astype(jnp.bfloat16)
            slope = gate + (0.5 * h) * (1.0 - tanh * tanh) * (GELU_A + 3.0 * GELU_B * square)
            grad_buf[lax.rem(i, 2), rows, :] = (grad_act * slope).astype(jnp.bfloat16)

        def back_down(i, n):
            j = tile_of(i)
            lanes = pl.ds(n * WIDTH, WIDTH)
            down = mm(act_buf[lax.rem(i, 2)], cot[s, :, lanes], 0, 0).reshape(SUB, 2, ROWS, WIDTH)
            own = jnp.where(core == 0, down[:, 0], down[:, 1])
            other = jnp.where(core == 0, down[:, 1], down[:, 0]).astype(jnp.bfloat16)
            rows = pl.ds(2 * lax.rem(j, 2), 2)
            for h in range(2):
                plane[t, lax.div(j, 2), rows, :, :, pl.ds(HALF + h * DIM + n * WIDTH, WIDTH)] = own[:, h * SUB:(h + 1) * SUB].reshape(2, RING, SUB, WIDTH)
            for k in range(SUB):
                gath[t, 1, 2 + lax.div(j, RING), lax.rem(j, RING), k // 2, :, pl.ds(k % 2 * DIM + n * WIDTH, WIDTH)] = other[k]

        def back_up(i, n, mine):
            up = mm(xbuf[slot, :, pl.ds(n * WIDTH, WIDTH)], grad_buf[lax.rem(i, 2)], 0, 0)
            cols = pl.ds(pl.multiple_of(lax.rem(tile_of(i), RING) * WIDTH, WIDTH), WIDTH)
            if mine:
                plane[t, pl.ds(2 * n, 2), :, :, :, cols] = up.reshape(2, RING, RING, SUB, WIDTH)
            else:
                gath[t, 1, n, :, :, :, cols] = up.astype(jnp.bfloat16).reshape(RING, RING, ROWS, WIDTH)

        def back_dx(i, m):
            rows = pl.ds(m * CHUNK, CHUNK)
            total[rows, :] = total[rows, :] + mm(grad_buf[lax.rem(i, 2), rows, :], wu[i], 1, 1)

        def events(k):
            if k == 3:
                tasks[t].run('up')
            advance(TILES * t + k)

        def tile(i, mine, ahead):
            if ahead:
                fetch(i + 1)
            for m in range(HALF // CHUNK):
                if ahead:
                    front(i + 1, m)
                for n in range(2):
                    if m == n * (HALF // CHUNK // 2):
                        back_down(i, n)
                        back_up(i, n, mine)
                if l == 1:
                    back_dx(i, m)
            if t < 3:
                for copy in weight_copies(t + 1, i):
                    copy.start()

        def segment(start, stop, mine):
            def body(i, carry):
                tile(i, mine, True)
                for k in range(start, stop):
                    if k == 3 or agenda and agenda[0][0] <= TILES * t + k:
                        @pl.when(i == k)
                        def _():
                            events(k)
                return carry

            lax.fori_loop(start, stop, body, 0)

        fetch(0)
        for m in range(HALF // CHUNK):
            front(0, m)
        segment(0, RING, False)
        segment(RING, TILES - 1, True)
        tile(TILES - 1, True, False)
        events(TILES - 1)
        if l == 1:
            cot[s] = (cot[s].astype(jnp.float32) + total[...]).astype(jnp.bfloat16)
        if t < 2:
            x_copy(t + 2).start()
        else:
            next_copy(t - 2).start()

    def forward(t, s, l, now):
        if l == 0:
            next_copy(s).wait()
        total[...] = jnp.zeros_like(total)

        def body(i, carry):
            half, lane = lax.div(i, 2), lax.rem(i, 2)
            lanes = pl.ds(pl.multiple_of(lane * WIDTH, WIDTH), WIDTH)
            raw = gath[t, half, :, :, :, :, lanes].astype(jnp.float32).reshape(RING ** 3, ROWS, WIDTH)
            ups, downs = [], []
            for q in range(2):
                ups.append(raw[:, q * SUB:(q + 1) * SUB].reshape(DIM, WIDTH).astype(jnp.bfloat16))
                rows = pl.ds(2 * lane, 2)
                even = gath[t, 0, 2 * half + q, rows, :, :, DIM:HALF].reshape(SUB, 1, ROWS, DIM)
                odd = gath[t, 1, 2 * half + q, rows, :, :, DIM:HALF].reshape(SUB, 1, ROWS, DIM)
                downs.append(jnp.concatenate([even, odd], axis=1).reshape(WIDTH, DIM))
            w1, w2 = jnp.concatenate(ups, axis=1), jnp.concatenate(downs, axis=0)
            count = HALF // SPAN
            hidden = mm(xbuf[s, 0:SPAN, :], w1, 1, 0)
            for m in range(count):
                h = hidden
                if m + 1 < count:
                    hidden = mm(xbuf[s, pl.ds((m + 1) * SPAN, SPAN), :], w1, 1, 0)
                tanh = jnp.tanh(h * (GELU_A + GELU_B * (h * h)))
                act = (h * (0.5 * tanh + 0.5)).astype(jnp.bfloat16)
                span = pl.ds(m * SPAN, SPAN)
                total[span, :] = total[span, :] + mm(act, w2, 1, 0)
            for k in range(RING):
                if agenda and agenda[0][0] <= now + k:
                    @pl.when(i == k)
                    def _():
                        advance(now + k)
            return carry

        lax.fori_loop(0, RING, body, 0)
        xbuf[s] = (xbuf[s].astype(jnp.float32) + total[...]).astype(jnp.bfloat16)
        if l == 1:
            y_copy(s).start()
        return now + RING

    for t in range(RING):
        backward(t)
    now = RING * TILES - 1
    for t, s, l in FORWARD:
        while (t, 12) not in finished:
            now = max(now, agenda[0][0])
            advance(agenda[0][0])
        now = forward(t, s, l, now)
    for s in range(2):
        y_copy(s).wait()


def fused_step(*args):
    vmem = pl.BlockSpec(memory_space=pltpu.VMEM)
    hbm = pl.BlockSpec(memory_space=pl.ANY)
    up_state = jax.ShapeDtypeStruct(args[5].shape, jnp.float32)
    down_state = jax.ShapeDtypeStruct(args[6].shape, jnp.float32)
    scratch = [
        pltpu.VMEM((TILES, DIM, WIDTH), jnp.bfloat16),
        pltpu.VMEM((TILES, WIDTH, DIM), jnp.bfloat16),
        pltpu.VMEM((2, HALF, DIM), jnp.bfloat16),
        pltpu.VMEM((2, HALF, DIM), jnp.bfloat16),
        pltpu.VMEM((HALF, DIM), jnp.float32),
        pltpu.VMEM((2, HALF, WIDTH), jnp.bfloat16),
        pltpu.VMEM((2, HALF, WIDTH), jnp.bfloat16),
        pltpu.VMEM((RING,) * RING + (SUB, FF), jnp.float32),
        pltpu.VMEM((2, 2, 2, RING, SUB, FF), jnp.float32),
        pltpu.VMEM((2, 2, RING, RING, SUB, FF), jnp.float32),
        pltpu.VMEM((2, 3, RING, SUB, FF), jnp.float32),
        pltpu.VMEM((RING, 3, SUB, FF), jnp.float32),
        pltpu.VMEM((RING, 2, SUB, HALF), jnp.float32),
        pltpu.VMEM((RING, 3, RING, HALF), jnp.float32),
        pltpu.VMEM((RING, SUB, FF), jnp.float32),
        pltpu.VMEM((RING, 2, RING, RING, RING, ROWS, HALF), jnp.bfloat16),
        pltpu.SemaphoreType.DMA((2, TILES)),
        pltpu.SemaphoreType.DMA((6,)),
        pltpu.SemaphoreType.DMA((RING, 66)),
        pltpu.SemaphoreType.DMA((RING, 66)),
        pltpu.SemaphoreType.REGULAR((2, 2, 3, 3)),
    ]
    return pl.pallas_call(
        step_kernel,
        out_shape=(up_state, down_state) * 3 + (jax.ShapeDtypeStruct(args[2].shape, jnp.bfloat16),),
        in_specs=[hbm] * 5 + [vmem] * SUB,
        out_specs=(vmem,) * 6 + (hbm,),
        scratch_shapes=scratch,
        compiler_params=pltpu.CompilerParams(collective_id=0, has_side_effects=True, vmem_limit_bytes=67043328),
        name='step',
    )(*args)


def finish_kernel(*refs):
    count = len(refs) // 3
    sources, results, stage, sem = refs[:count], refs[count:2 * count], refs[2 * count:3 * count], refs[3 * count]
    inward = [pltpu.make_async_copy(sources[i], stage[i], sem.at[0, i]) for i in range(count)]
    outward = [pltpu.make_async_copy(stage[i], results[i], sem.at[1, i]) for i in range(count)]
    for copy in inward:
        copy.start()
    for i in range(count):
        inward[i].wait()
        outward[i].start()
    for copy in outward:
        copy.wait()


def finish(parts):
    hbm = pl.BlockSpec(memory_space=pl.ANY)
    return pl.pallas_call(
        finish_kernel,
        out_shape=tuple(jax.ShapeDtypeStruct(part.shape, part.dtype) for part in parts),
        in_specs=[hbm] * len(parts),
        out_specs=(hbm,) * len(parts),
        scratch_shapes=[pltpu.VMEM(part.shape, part.dtype) for part in parts] + [pltpu.SemaphoreType.DMA((2, len(parts)))],
        name='finish',
    )(*parts)


def solution(mesh):
    tok_spec = P(None, 'fsdp')
    layer_spec = P(None, None, 'fsdp')
    rep_spec = P()

    def device_step(*args):
        return tuple(finish(fused_step(*args)))

    return jax.shard_map(device_step, mesh=mesh, in_specs=(layer_spec, tok_spec, tok_spec, rep_spec, rep_spec) + (layer_spec,) * SUB, out_specs=(layer_spec,) * 6 + (tok_spec,), check_vma=False)
```

```python
import jax
import jax.numpy as jnp
from jax import lax
from jax.experimental import pallas as pl
from jax.experimental.pallas import tpu as pltpu
from jax.sharding import PartitionSpec as P

LEARN_RATE = 0.005
BETA_ONE = 0.9
BETA_TWO = 0.95
ADAM_EPS = 1e-8
WEIGHT_DECAY = 0.1
MICROBATCHES = 2
ADAM_STEP = 2
MESH = pl.DeviceIdType.MESH

ORDERS = ((2, 1, 0), (1, 0, 2), (0, 2, 1))
RS_LANES = (((0, 384), (384, 384), (768, 256)), ((1024, 384), (1408, 256), (1664, 384)))
AG_LANES = (((0, 128), (128, 128), (256, 256)), ((512, 128), (640, 256), (896, 128)))
TASKS = ((0, 1), (0, 0), (1, 1), (1, 0))
TILES = 8
CHUNK = 512
SPAN = 256
RING = 4
SUB = 8
ROWS = 16
DIM = 512
HALF = 1024
FF = 2048
WIDTH = 256
GATHER_LAG = 4
OFFSETS = ((0, 3, 8, 13, 18, 19, 20, 24, 28, 34, 38, 42),
           (2, 6, 13, 18, 22, None, None, 26, 30, 36, 40, 44))
FORWARD = ((1, 0, 0), (0, 0, 1), (3, 1, 0), (2, 1, 1))
GELU_A = 0.7978845608028654
GELU_B = GELU_A * 0.044715


def adam_update(acc_part, grad_new, master, moment_one, moment_two):
    grad_mean = (acc_part + grad_new) / MICROBATCHES
    moment_one = BETA_ONE * moment_one + (1.0 - BETA_ONE) * grad_mean
    moment_two = BETA_TWO * moment_two + (1.0 - BETA_TWO) * grad_mean * grad_mean
    corr_one = 1.0 - BETA_ONE ** ADAM_STEP
    corr_two = 1.0 - BETA_TWO ** ADAM_STEP
    step_dir = (moment_one / corr_one) / (jnp.sqrt(moment_two / corr_two) + ADAM_EPS)
    master = master - LEARN_RATE * (step_dir + WEIGHT_DECAY * master)
    return master, moment_one, moment_two


def mm(a, b, a_dim, b_dim):
    return lax.dot_general(a, b, (((a_dim,), (b_dim,)), ((), ())), preferred_element_type=jnp.float32)


def half_dim(axis):
    return 1 if axis == 0 else 0


def region(fixed, lanes):
    return tuple(fixed.get(dim, slice(None)) for dim in range(3)) + (slice(None), pl.ds(lanes[0], lanes[1]))


def step_kernel(*refs):
    x_saved, grad_out, x_next, w_up, w_down = refs[0:5]
    acc_up, acc_down, master_up, master_down, m1_up, m1_down, m2_up, m2_down = refs[5:13]
    out_states = refs[13:19]
    y_out = refs[19]
    (wu, wd, xbuf, cot, total, act_buf, grad_buf, plane, rs1, rs2, rs3, rs4, grad_x, part_x, block8, gath, w_sem, x_sem, send_sem, recv_sem, free_sem) = refs[20:]

    me = lax.axis_index('fsdp')
    core = lax.rem(me, 2)
    chip = lax.div(me, 2)
    pos = (lax.div(chip, ROWS), lax.rem(lax.div(chip, RING), RING), lax.rem(chip, RING))
    stride = (32, SUB, 2)
    partner = me + 1 - 2 * core
    near_z, far_z = 2 + core, 3 - core
    near = [[lax.rem(pos[axis] + step, RING) for step in range(RING)] for axis in range(3)]
    peers = [[me + (near[axis][step] - pos[axis]) * stride[axis] for step in range(RING)] for axis in range(3)]

    def tile_of(i):
        return lax.rem(i + RING * (1 - core), TILES)

    def weight_copies(t, i):
        s, l = TASKS[t]
        cols = pl.ds(pl.multiple_of(tile_of(i) * WIDTH, WIDTH), WIDTH)
        return (pltpu.make_async_copy(w_up.at[s, l, :, cols], wu.at[i], w_sem.at[0, i]),
                pltpu.make_async_copy(w_down.at[s, l, cols, :], wd.at[i], w_sem.at[1, i]))

    def x_copy(t):
        s, l = TASKS[t]
        return pltpu.make_async_copy(x_saved.at[s, l, 0], xbuf.at[t % 2], x_sem.at[t % 2])

    def next_copy(s):
        return pltpu.make_async_copy(x_next.at[s, 0], xbuf.at[s], x_sem.at[s])

    def cot_copy(s):
        return pltpu.make_async_copy(grad_out.at[s, 0], cot.at[s], x_sem.at[2 + s])

    def y_copy(s):
        return pltpu.make_async_copy(xbuf.at[s], y_out.at[s, 0], x_sem.at[RING + s])

    x_copy(0).start()
    cot_copy(0).start()

    def first_weights(i, carry):
        for copy in weight_copies(0, i):
            copy.start()
        return carry

    lax.fori_loop(0, TILES, first_weights, 0)
    x_copy(1).start()
    cot_copy(1).start()

    barrier = pltpu.get_barrier_semaphore()
    pl.semaphore_signal(barrier, inc=1, device_id=(partner,), device_id_type=MESH)
    for axis in range(3):
        for step in (1, 2, 3):
            pl.semaphore_signal(barrier, inc=1, device_id=(peers[axis][step],), device_id_type=MESH)
    pl.semaphore_wait(barrier, 10)

    class Chain:
        def __init__(self, task_id, part):
            self.t = task_id
            self.par = task_id % 2
            self.part = part
            self.row = 2 * task_id + part
            self.slot = 0
            self.live = []
            self.stage, self.layer = TASKS[task_id]
            turn = [ORDERS[(g + task_id) % 3] for g in range(3)]
            self.groups = [(g, turn[g], RS_LANES[part][g], AG_LANES[part][g]) for g in range(3)]

        def send(self, src, dst, device):
            slot = self.slot
            self.slot += 1
            index = len(self.live)

            def make():
                return pltpu.make_async_remote_copy(src_ref=src(), dst_ref=dst(), send_sem=send_sem.at[self.row, index], recv_sem=recv_sem.at[self.row, slot], device_id=(device,), device_id_type=MESH)

            make().start()
            self.live.append(make)

        def drain(self):
            for make in self.live:
                make().wait()
            self.live = []

        def plane_at(self, fixed, span):
            return lambda: plane.at[(self.t,) + region(fixed, span)]

        def gath_at(self, fixed, span):
            return lambda: gath.at[(self.t, core) + region(fixed, span)]

        def run(self, phase):
            getattr(self, 'phase_%s' % phase)()

        def pass_half(self, z_blk):
            self.send(lambda: gath.at[self.t, 1, z_blk], lambda: gath.at[self.t, 0, z_blk], partner)

        def early(self):
            self.pass_half(far_z if self.part else pl.ds(0, 2))

        def late(self):
            if self.part:
                self.pass_half(near_z)

        def phase_1(self):
            t, par = self.t, self.par
            self.drain()

            def body(i, carry):
                z_pos, y_pos = lax.div(i, RING), lax.rem(i, RING)
                z_blk, y_blk, x_blk = lax.div(i, SUB), lax.div(lax.rem(i, SUB), 2), 2 * lax.rem(i, 2)
                got = gath[t, 0, z_blk + 2 * self.part, y_blk, pl.ds(x_blk, 2)].astype(jnp.float32)
                if self.part == 0:
                    plane[t, z_pos, y_pos, :, :, 0:HALF] = plane[t, z_pos, y_pos, :, :, 0:HALF] + got.reshape(RING, SUB, HALF)
                else:
                    for k in range(2):
                        for m in range(2):
                            for h in range(2):
                                lanes = slice(HALF + DIM * h, HALF + DIM * (h + 1))
                                plane[t, z_pos, y_pos, 2 * k + m, :, lanes] = plane[t, z_pos, y_pos, 2 * k + m, :, lanes] + got[k, SUB * h:SUB * (h + 1), DIM * m:DIM * (m + 1)]
                return carry

            lax.fori_loop(0, ROWS, body, 0)
            for g, order, span, _ in self.groups:
                axis, half = order[0], half_dim(order[0])
                lanes = pl.ds(*span)
                for way, step in ((0, 1), (1, 3)):
                    self.send(self.plane_at({axis: near[axis][2], half: pl.ds(2 * way, 2)}, span), lambda way=way, lanes=lanes: rs1.at[par, way, :, :, :, lanes], peers[axis][step])

        def phase_2(self):
            t, par = self.t, self.par
            self.drain()
            for g, order, span, _ in self.groups:
                axis, half = order[0], half_dim(order[0])
                lanes = pl.ds(*span)
                for way, step in ((0, 1), (1, 3)):
                    where = (t,) + region({axis: near[axis][step], half: pl.ds(2 * way, 2)}, span)
                    plane[where] = plane[where] + rs1[par, way, :, :, :, lanes]
            for g, order, span, _ in self.groups:
                axis = order[0]
                lanes = pl.ds(*span)
                for way, step in ((0, 1), (1, 3)):
                    if t >= 2:
                        pl.semaphore_wait(free_sem.at[0, par, self.part, g, way], 1)
                    self.send(self.plane_at({axis: near[axis][step]}, span), lambda way=way, lanes=lanes: rs2.at[par, way, :, :, :, lanes], peers[axis][step])

        def phase_3(self):
            t, par = self.t, self.par
            self.drain()
            for g, order, span, _ in self.groups:
                lanes = pl.ds(*span)
                where = (t,) + region({order[0]: pos[order[0]]}, span)
                plane[where] = plane[where] + (rs2[par, 0, :, :, :, lanes] + rs2[par, 1, :, :, :, lanes])
                if t < 2:
                    for way, step in ((0, 3), (1, 1)):
                        pl.semaphore_signal(free_sem.at[0, par, self.part, g, way], inc=1, device_id=(peers[order[0]][step],), device_id_type=MESH)
            for g, order, span, _ in self.groups:
                lanes = pl.ds(*span)
                axis = order[1]
                for step in (1, 2, 3):
                    if t >= 2:
                        pl.semaphore_wait(free_sem.at[1, par, self.part, g, step - 1], 1)
                    self.send(self.plane_at({order[0]: pos[order[0]], axis: near[axis][step]}, span), lambda step=step, lanes=lanes: rs3.at[par, step - 1, :, :, lanes], peers[axis][step])

        def phase_4(self):
            t, par = self.t, self.par
            self.drain()
            for g, order, span, _ in self.groups:
                lanes = pl.ds(*span)
                where = (t,) + region({order[0]: pos[order[0]], order[1]: pos[order[1]]}, span)
                plane[where] = plane[where] + (rs3[par, 0, :, :, lanes] + rs3[par, 1, :, :, lanes] + rs3[par, 2, :, :, lanes])
                if t < 2:
                    for step in (1, 2, 3):
                        pl.semaphore_signal(free_sem.at[1, par, self.part, g, step - 1], inc=1, device_id=(peers[order[1]][RING - step],), device_id_type=MESH)
            for g, order, span, _ in self.groups:
                lanes = pl.ds(*span)
                axis = order[2]
                fixed = {order[0]: pos[order[0]], order[1]: pos[order[1]]}
                for step in (1, 2, 3):
                    self.send(self.plane_at({**fixed, axis: near[axis][step]}, span), lambda step=step, lanes=lanes: rs4.at[t, step - 1, :, lanes], peers[axis][step])

        def phase_5(self):
            t = self.t
            self.drain()
            lanes = slice(HALF * self.part, HALF * (self.part + 1))
            block = plane[t, pos[0], pos[1], pos[2], :, lanes] + (rs4[t, 0, :, lanes] + rs4[t, 1, :, lanes] + rs4[t, 2, :, lanes])
            if self.part == 0:
                grad_x[t, core] = block
                self.send(lambda: grad_x.at[t, core], lambda: grad_x.at[t, core], partner)
            else:
                s, l = self.stage, self.layer
                grad = jnp.concatenate([block[:, 0:DIM], block[:, DIM:HALF]], axis=0)
                new = adam_update(acc_down[s, l], grad, master_down[s, l], m1_down[s, l], m2_down[s, l])
                for i in range(3):
                    out_states[2 * i + 1][s, l] = new[i]
                gath[t, core, pos[0], pos[1], pos[2], :, DIM:HALF] = new[0].astype(jnp.bfloat16)
                self.spread()

        def phase_6(self):
            t, s, l = self.t, self.stage, self.layer
            self.drain()
            low = jnp.concatenate([grad_x[t, 0, 0:RING, :], grad_x[t, 1, 0:RING, :]], axis=1)
            high = jnp.concatenate([grad_x[t, 0, RING:SUB, :], grad_x[t, 1, RING:SUB, :]], axis=1)
            grad_up = jnp.where(core == 0, low, high)
            new_up = adam_update(acc_up[s, l], grad_up, master_up[s, l], m1_up[s, l], m2_up[s, l])
            for i in range(3):
                out_states[2 * i][s, l] = new_up[i]
            left, right = new_up[0][:, 0:HALF], new_up[0][:, HALF:FF]
            part_x[t, core] = jnp.where(core == 0, left, right)
            part_x[t, 2] = jnp.where(core == 0, right, left)
            self.send(lambda: part_x.at[t, 2], lambda: part_x.at[t, core], partner)

        def phase_7(self):
            t = self.t
            self.drain()
            block8[t, 0:RING, :] = part_x[t, 0]
            block8[t, RING:SUB, :] = part_x[t, 1]
            rows = jnp.concatenate([block8[t, :, 0:DIM], block8[t, :, DIM:HALF]], axis=0)
            gath[t, core, pos[0], pos[1], pos[2], :, 0:DIM] = rows.astype(jnp.bfloat16)
            self.spread()

        def spread(self):
            for g, order, _, span in self.groups:
                where = self.gath_at({0: pos[0], 1: pos[1], 2: pos[2]}, span)
                for step in (1, 2, 3):
                    self.send(where, where, peers[order[2]][step])

        def phase_8(self):
            self.drain()
            for g, order, _, span in self.groups:
                where = self.gath_at({order[0]: pos[order[0]], order[1]: pos[order[1]]}, span)
                for step in (1, 2, 3):
                    self.send(where, where, peers[order[1]][step])

        def phase_9(self):
            self.drain()
            for g, order, _, span in self.groups:
                where = self.gath_at({order[0]: pos[order[0]]}, span)
                for step in (1, 3):
                    self.send(where, where, peers[order[0]][step])

        def phase_10(self):
            self.drain()
            for g, order, _, span in self.groups:
                axis, half = order[0], half_dim(order[0])
                for way, step in ((0, 1), (1, 3)):
                    where = self.gath_at({axis: near[axis][RING - step], half: pl.ds(2 * way, 2)}, span)
                    self.send(where, where, peers[axis][step])

        def phase_11(self):
            self.drain()
            lanes = pl.ds(DIM * self.part, DIM)
            whole = lambda: gath.at[self.t, core, :, :, :, :, lanes]
            self.send(whole, whole, partner)

        def phase_12(self):
            self.drain()

    chains = [[Chain(t, part) for part in range(2)] for t in range(RING)]
    agenda = sorted((TILES * (t + 1) - 1 + offset + (GATHER_LAG * (3 - t) if phase > 5 else 0), t, part, phase + 1) for t in range(RING) for part in range(2) for phase, offset in enumerate(OFFSETS[part]) if offset is not None)
    finished = set()

    def advance(now):
        while agenda and agenda[0][0] <= now:
            _, t, part, phase = agenda.pop(0)
            chains[t][part].run(phase)
            finished.add((t, part, phase))

    def backward(t):
        s, l = TASKS[t]
        slot = t % 2
        x_copy(t).wait()
        if l == 1:
            cot_copy(s).wait()
            total[...] = jnp.zeros_like(total)

        def fetch(i):
            for copy in weight_copies(t, i):
                copy.wait()

        def front(i, m):
            rows = pl.ds(m * CHUNK, CHUNK)
            h = mm(xbuf[slot, rows, :], wu[i], 1, 0)
            grad_act = mm(cot[s, rows, :], wd[i], 1, 1)
            square = h * h
            tanh = jnp.tanh(h * (GELU_A + GELU_B * square))
            gate = 0.5 * tanh + 0.5
            act_buf[lax.rem(i, 2), rows, :] = (h * gate).astype(jnp.bfloat16)
            slope = gate + (0.5 * h) * (1.0 - tanh * tanh) * (GELU_A + 3.0 * GELU_B * square)
            grad_buf[lax.rem(i, 2), rows, :] = (grad_act * slope).astype(jnp.bfloat16)

        def back_down(i, n):
            j = tile_of(i)
            lanes = pl.ds(n * WIDTH, WIDTH)
            down = mm(act_buf[lax.rem(i, 2)], cot[s, :, lanes], 0, 0).reshape(SUB, 2, ROWS, WIDTH)
            own = jnp.where(core == 0, down[:, 0], down[:, 1])
            other = jnp.where(core == 0, down[:, 1], down[:, 0]).astype(jnp.bfloat16)
            rows = pl.ds(2 * lax.rem(j, 2), 2)
            for h in range(2):
                plane[t, lax.div(j, 2), rows, :, :, pl.ds(HALF + h * DIM + n * WIDTH, WIDTH)] = own[:, h * SUB:(h + 1) * SUB].reshape(2, RING, SUB, WIDTH)
            for k in range(SUB):
                gath[t, 1, 2 + lax.div(j, RING), lax.rem(j, RING), k // 2, :, pl.ds(k % 2 * DIM + n * WIDTH, WIDTH)] = other[k]

        def back_up(i, n, mine):
            up = mm(xbuf[slot, :, pl.ds(n * WIDTH, WIDTH)], grad_buf[lax.rem(i, 2)], 0, 0)
            cols = pl.ds(pl.multiple_of(lax.rem(tile_of(i), RING) * WIDTH, WIDTH), WIDTH)
            if mine:
                plane[t, pl.ds(2 * n, 2), :, :, :, cols] = up.reshape(2, RING, RING, SUB, WIDTH)
            else:
                gath[t, 1, n, :, :, :, cols] = up.astype(jnp.bfloat16).reshape(RING, RING, ROWS, WIDTH)

        def back_dx(i, m):
            rows = pl.ds(m * CHUNK, CHUNK)
            total[rows, :] = total[rows, :] + mm(grad_buf[lax.rem(i, 2), rows, :], wu[i], 1, 1)

        def events(k):
            if k == 3:
                for chain in chains[t]:
                    chain.early()
            if k == TILES - 1:
                for chain in chains[t]:
                    chain.late()
            advance(TILES * t + k)

        def tile(i, mine, ahead):
            if ahead:
                fetch(i + 1)
            for m in range(HALF // CHUNK):
                if ahead:
                    front(i + 1, m)
                for n in range(2):
                    if m == n * (HALF // CHUNK // 2):
                        back_down(i, n)
                        back_up(i, n, mine)
                if l == 1:
                    back_dx(i, m)
            if t < 3:
                for copy in weight_copies(t + 1, i):
                    copy.start()

        def segment(start, stop, mine):
            def body(i, carry):
                tile(i, mine, True)
                for k in range(start, stop):
                    if k == 3 or agenda and agenda[0][0] <= TILES * t + k:
                        @pl.when(i == k)
                        def _():
                            events(k)
                return carry

            lax.fori_loop(start, stop, body, 0)

        fetch(0)
        for m in range(HALF // CHUNK):
            front(0, m)
        segment(0, RING, False)
        segment(RING, TILES - 1, True)
        tile(TILES - 1, True, False)
        events(TILES - 1)
        if l == 1:
            cot[s] = (cot[s].astype(jnp.float32) + total[...]).astype(jnp.bfloat16)
        if t < 2:
            x_copy(t + 2).start()
        else:
            next_copy(t - 2).start()

    def forward(t, s, l, now):
        if l == 0:
            next_copy(s).wait()
        total[...] = jnp.zeros_like(total)

        def body(i, carry):
            half, lane = lax.div(i, 2), lax.rem(i, 2)
            lanes = pl.ds(pl.multiple_of(lane * WIDTH, WIDTH), WIDTH)
            raw = gath[t, half, :, :, :, :, lanes].astype(jnp.float32).reshape(RING ** 3, ROWS, WIDTH)
            ups, downs = [], []
            for q in range(2):
                ups.append(raw[:, q * SUB:(q + 1) * SUB].reshape(DIM, WIDTH).astype(jnp.bfloat16))
                rows = pl.ds(2 * lane, 2)
                even = gath[t, 0, 2 * half + q, rows, :, :, DIM:HALF].reshape(SUB, 1, ROWS, DIM)
                odd = gath[t, 1, 2 * half + q, rows, :, :, DIM:HALF].reshape(SUB, 1, ROWS, DIM)
                downs.append(jnp.concatenate([even, odd], axis=1).reshape(WIDTH, DIM))
            w1, w2 = jnp.concatenate(ups, axis=1), jnp.concatenate(downs, axis=0)
            count = HALF // SPAN
            hidden = mm(xbuf[s, 0:SPAN, :], w1, 1, 0)
            for m in range(count):
                h = hidden
                if m + 1 < count:
                    hidden = mm(xbuf[s, pl.ds((m + 1) * SPAN, SPAN), :], w1, 1, 0)
                tanh = jnp.tanh(h * (GELU_A + GELU_B * (h * h)))
                act = (h * (0.5 * tanh + 0.5)).astype(jnp.bfloat16)
                span = pl.ds(m * SPAN, SPAN)
                total[span, :] = total[span, :] + mm(act, w2, 1, 0)
            for k in range(RING):
                if agenda and agenda[0][0] <= now + k:
                    @pl.when(i == k)
                    def _():
                        advance(now + k)
            return carry

        lax.fori_loop(0, RING, body, 0)
        xbuf[s] = (xbuf[s].astype(jnp.float32) + total[...]).astype(jnp.bfloat16)
        if l == 1:
            y_copy(s).start()
        return now + RING

    for t in range(RING):
        backward(t)
    now = RING * TILES - 1
    for t, s, l in FORWARD:
        while not finished >= {(t, 0, 12), (t, 1, 12)}:
            now = max(now, agenda[0][0])
            advance(agenda[0][0])
        now = forward(t, s, l, now)
    for s in range(2):
        y_copy(s).wait()


def fused_step(*args):
    vmem = pl.BlockSpec(memory_space=pltpu.VMEM)
    hbm = pl.BlockSpec(memory_space=pl.ANY)
    up_state = jax.ShapeDtypeStruct(args[5].shape, jnp.float32)
    down_state = jax.ShapeDtypeStruct(args[6].shape, jnp.float32)
    scratch = [
        pltpu.VMEM((TILES, DIM, WIDTH), jnp.bfloat16),
        pltpu.VMEM((TILES, WIDTH, DIM), jnp.bfloat16),
        pltpu.VMEM((2, HALF, DIM), jnp.bfloat16),
        pltpu.VMEM((2, HALF, DIM), jnp.bfloat16),
        pltpu.VMEM((HALF, DIM), jnp.float32),
        pltpu.VMEM((2, HALF, WIDTH), jnp.bfloat16),
        pltpu.VMEM((2, HALF, WIDTH), jnp.bfloat16),
        pltpu.VMEM((RING,) * RING + (SUB, FF), jnp.float32),
        pltpu.VMEM((2, 2, 2, RING, SUB, FF), jnp.float32),
        pltpu.VMEM((2, 2, RING, RING, SUB, FF), jnp.float32),
        pltpu.VMEM((2, 3, RING, SUB, FF), jnp.float32),
        pltpu.VMEM((RING, 3, SUB, FF), jnp.float32),
        pltpu.VMEM((RING, 2, SUB, HALF), jnp.float32),
        pltpu.VMEM((RING, 3, RING, HALF), jnp.float32),
        pltpu.VMEM((RING, SUB, HALF), jnp.float32),
        pltpu.VMEM((RING, 2, RING, RING, RING, ROWS, HALF), jnp.bfloat16),
        pltpu.SemaphoreType.DMA((2, TILES)),
        pltpu.SemaphoreType.DMA((6,)),
        pltpu.SemaphoreType.DMA((SUB, 9)),
        pltpu.SemaphoreType.DMA((SUB, 66)),
        pltpu.SemaphoreType.REGULAR((2, 2, 2, 3, 3)),
    ]
    return pl.pallas_call(
        step_kernel,
        out_shape=(up_state, down_state) * 3 + (jax.ShapeDtypeStruct(args[2].shape, jnp.bfloat16),),
        in_specs=[hbm] * 5 + [vmem] * SUB,
        out_specs=(vmem,) * 6 + (hbm,),
        scratch_shapes=scratch,
        compiler_params=pltpu.CompilerParams(collective_id=0, has_side_effects=True, vmem_limit_bytes=67043328),
        name='step',
    )(*args)


def finish_kernel(*refs):
    count = len(refs) // 3
    sources, results, stage, sem = refs[:count], refs[count:2 * count], refs[2 * count:3 * count], refs[3 * count]
    inward = [pltpu.make_async_copy(sources[i], stage[i], sem.at[0, i]) for i in range(count)]
    outward = [pltpu.make_async_copy(stage[i], results[i], sem.at[1, i]) for i in range(count)]
    for copy in inward:
        copy.start()
    for i in range(count):
        inward[i].wait()
        outward[i].start()
    for copy in outward:
        copy.wait()


def finish(parts):
    hbm = pl.BlockSpec(memory_space=pl.ANY)
    return pl.pallas_call(
        finish_kernel,
        out_shape=tuple(jax.ShapeDtypeStruct(part.shape, part.dtype) for part in parts),
        in_specs=[hbm] * len(parts),
        out_specs=(hbm,) * len(parts),
        scratch_shapes=[pltpu.VMEM(part.shape, part.dtype) for part in parts] + [pltpu.SemaphoreType.DMA((2, len(parts)))],
        name='finish',
    )(*parts)


def solution(mesh):
    tok_spec = P(None, 'fsdp')
    layer_spec = P(None, None, 'fsdp')
    rep_spec = P()

    def device_step(*args):
        return tuple(finish(fused_step(*args)))

    return jax.shard_map(device_step, mesh=mesh, in_specs=(layer_spec, tok_spec, tok_spec, rep_spec, rep_spec) + (layer_spec,) * SUB, out_specs=(layer_spec,) * 6 + (tok_spec,), check_vma=False)
```

```python
import jax
import jax.numpy as jnp
from jax import lax
from jax.experimental import pallas as pl
from jax.experimental.pallas import tpu as pltpu
from jax.sharding import PartitionSpec as P

LEARN_RATE = 0.005
BETA_ONE = 0.9
BETA_TWO = 0.95
ADAM_EPS = 1e-8
WEIGHT_DECAY = 0.1
MICROBATCHES = 2
ADAM_STEP = 2
MESH = pl.DeviceIdType.MESH

ORDERS = ((2, 1, 0), (1, 0, 2), (0, 2, 1))
RS_LANES = (((0, 384), (384, 384), (768, 256)), ((1024, 384), (1408, 256), (1664, 384)))
AG_LANES = (((0, 128), (128, 128), (256, 256)), ((512, 128), (640, 256), (896, 128)))
TASKS = ((0, 1), (0, 0), (1, 1), (1, 0))
TILES = 8
CHUNK = 512
SPAN = 512
RING = 4
SUB = 8
ROWS = 16
DIM = 512
HALF = 1024
FF = 2048
WIDTH = 256
GATHER_LAG = 4
OFFSETS = ((0, 3, 8, 13, 17, 18, 19, 22, 26, 31, 35, 39),
           (1, 5, 11, 16, 20, None, None, 24, 28, 33, 37, 41))
FORWARD = ((1, 0, 0), (0, 0, 1), (3, 1, 0), (2, 1, 1))
GELU_A = 0.7978845608028654
GELU_B = GELU_A * 0.044715


def adam_update(acc_part, grad_new, master, moment_one, moment_two):
    grad_mean = (acc_part + grad_new) / MICROBATCHES
    moment_one = BETA_ONE * moment_one + (1.0 - BETA_ONE) * grad_mean
    moment_two = BETA_TWO * moment_two + (1.0 - BETA_TWO) * grad_mean * grad_mean
    corr_one = 1.0 - BETA_ONE ** ADAM_STEP
    corr_two = 1.0 - BETA_TWO ** ADAM_STEP
    step_dir = (moment_one / corr_one) / (jnp.sqrt(moment_two / corr_two) + ADAM_EPS)
    master = master - LEARN_RATE * (step_dir + WEIGHT_DECAY * master)
    return master, moment_one, moment_two


def mm(a, b, a_dim, b_dim):
    return lax.dot_general(a, b, (((a_dim,), (b_dim,)), ((), ())), preferred_element_type=jnp.float32)


def half_dim(axis):
    return 1 if axis == 0 else 0


def region(fixed, lanes):
    return tuple(fixed.get(dim, slice(None)) for dim in range(3)) + (slice(None), pl.ds(lanes[0], lanes[1]))


def step_kernel(*refs):
    x_saved, grad_out, x_next, w_up, w_down = refs[0:5]
    acc_up, acc_down, master_up, master_down, m1_up, m1_down, m2_up, m2_down = refs[5:13]
    out_states = refs[13:19]
    y_out = refs[19]
    (wu, wd, xbuf, cot, total, act_buf, grad_buf, plane, rs1, rs2, rs3, rs4, grad_x, part_x, block8, gath, w_sem, x_sem, send_sem, recv_sem, free_sem) = refs[20:]

    me = lax.axis_index('fsdp')
    core = lax.rem(me, 2)
    chip = lax.div(me, 2)
    pos = (lax.div(chip, ROWS), lax.rem(lax.div(chip, RING), RING), lax.rem(chip, RING))
    stride = (32, SUB, 2)
    partner = me + 1 - 2 * core
    near_z, far_z = 2 + core, 3 - core
    near = [[lax.rem(pos[axis] + step, RING) for step in range(RING)] for axis in range(3)]
    peers = [[me + (near[axis][step] - pos[axis]) * stride[axis] for step in range(RING)] for axis in range(3)]

    def tile_of(i):
        return lax.rem(i + RING * (1 - core), TILES)

    def weight_copies(t, i):
        s, l = TASKS[t]
        cols = pl.ds(pl.multiple_of(tile_of(i) * WIDTH, WIDTH), WIDTH)
        return (pltpu.make_async_copy(w_up.at[s, l, :, cols], wu.at[i], w_sem.at[0, i]),
                pltpu.make_async_copy(w_down.at[s, l, cols, :], wd.at[i], w_sem.at[1, i]))

    def x_copy(t):
        s, l = TASKS[t]
        return pltpu.make_async_copy(x_saved.at[s, l, 0], xbuf.at[t % 2], x_sem.at[t % 2])

    def next_copy(s):
        return pltpu.make_async_copy(x_next.at[s, 0], xbuf.at[s], x_sem.at[s])

    def cot_copy(s):
        return pltpu.make_async_copy(grad_out.at[s, 0], cot.at[s], x_sem.at[2 + s])

    def y_copy(s):
        return pltpu.make_async_copy(xbuf.at[s], y_out.at[s, 0], x_sem.at[RING + s])

    x_copy(0).start()
    cot_copy(0).start()

    def first_weights(i, carry):
        for copy in weight_copies(0, i):
            copy.start()
        return carry

    lax.fori_loop(0, TILES, first_weights, 0)
    x_copy(1).start()
    cot_copy(1).start()

    barrier = pltpu.get_barrier_semaphore()
    pl.semaphore_signal(barrier, inc=1, device_id=(partner,), device_id_type=MESH)
    for axis in range(3):
        for step in (1, 2, 3):
            pl.semaphore_signal(barrier, inc=1, device_id=(peers[axis][step],), device_id_type=MESH)
    pl.semaphore_wait(barrier, 10)

    class Chain:
        def __init__(self, task_id, part):
            self.t = task_id
            self.par = task_id % 2
            self.part = part
            self.row = 2 * task_id + part
            self.slot = 0
            self.live = []
            self.stage, self.layer = TASKS[task_id]
            turn = [ORDERS[(g + task_id) % 3] for g in range(3)]
            self.groups = [(g, turn[g], RS_LANES[part][g], AG_LANES[part][g]) for g in range(3)]

        def send(self, src, dst, device):
            slot = self.slot
            self.slot += 1
            index = len(self.live)

            def make():
                return pltpu.make_async_remote_copy(src_ref=src(), dst_ref=dst(), send_sem=send_sem.at[self.row, index], recv_sem=recv_sem.at[self.row, slot], device_id=(device,), device_id_type=MESH)

            make().start()
            self.live.append(make)

        def drain(self):
            for make in self.live:
                make().wait()
            self.live = []

        def plane_at(self, fixed, span):
            return lambda: plane.at[(self.t,) + region(fixed, span)]

        def gath_at(self, fixed, span):
            return lambda: gath.at[(self.t, core) + region(fixed, span)]

        def run(self, phase):
            getattr(self, 'phase_%s' % phase)()

        def pass_half(self, z_blk):
            self.send(lambda: gath.at[self.t, 1, z_blk], lambda: gath.at[self.t, 0, z_blk], partner)

        def early(self):
            self.pass_half(far_z if self.part else pl.ds(0, 2))

        def late(self):
            if self.part:
                self.pass_half(near_z)

        def phase_1(self):
            t, par = self.t, self.par
            self.drain()

            def body(i, carry):
                z_pos, y_pos = lax.div(i, RING), lax.rem(i, RING)
                z_blk, y_blk, x_blk = lax.div(i, SUB), lax.div(lax.rem(i, SUB), 2), 2 * lax.rem(i, 2)
                got = gath[t, 0, z_blk + 2 * self.part, y_blk, pl.ds(x_blk, 2)].astype(jnp.float32)
                if self.part == 0:
                    plane[t, z_pos, y_pos, :, :, 0:HALF] = plane[t, z_pos, y_pos, :, :, 0:HALF] + got.reshape(RING, SUB, HALF)
                else:
                    for k in range(2):
                        for m in range(2):
                            for h in range(2):
                                lanes = slice(HALF + DIM * h, HALF + DIM * (h + 1))
                                plane[t, z_pos, y_pos, 2 * k + m, :, lanes] = plane[t, z_pos, y_pos, 2 * k + m, :, lanes] + got[k, SUB * h:SUB * (h + 1), DIM * m:DIM * (m + 1)]
                return carry

            lax.fori_loop(0, ROWS, body, 0)
            for g, order, span, _ in self.groups:
                axis, half = order[0], half_dim(order[0])
                lanes = pl.ds(*span)
                for way, step in ((0, 1), (1, 3)):
                    self.send(self.plane_at({axis: near[axis][2], half: pl.ds(2 * way, 2)}, span), lambda way=way, lanes=lanes: rs1.at[par, way, :, :, :, lanes], peers[axis][step])

        def phase_2(self):
            t, par = self.t, self.par
            self.drain()
            for g, order, span, _ in self.groups:
                axis, half = order[0], half_dim(order[0])
                lanes = pl.ds(*span)
                for way, step in ((0, 1), (1, 3)):
                    where = (t,) + region({axis: near[axis][step], half: pl.ds(2 * way, 2)}, span)
                    plane[where] = plane[where] + rs1[par, way, :, :, :, lanes]
            for g, order, span, _ in self.groups:
                axis = order[0]
                lanes = pl.ds(*span)
                for way, step in ((0, 1), (1, 3)):
                    if t >= 2:
                        pl.semaphore_wait(free_sem.at[0, par, self.part, g, way], 1)
                    self.send(self.plane_at({axis: near[axis][step]}, span), lambda way=way, lanes=lanes: rs2.at[par, way, :, :, :, lanes], peers[axis][step])

        def phase_3(self):
            t, par = self.t, self.par
            self.drain()
            for g, order, span, _ in self.groups:
                lanes = pl.ds(*span)
                where = (t,) + region({order[0]: pos[order[0]]}, span)
                plane[where] = plane[where] + (rs2[par, 0, :, :, :, lanes] + rs2[par, 1, :, :, :, lanes])
                if t < 2:
                    for way, step in ((0, 3), (1, 1)):
                        pl.semaphore_signal(free_sem.at[0, par, self.part, g, way], inc=1, device_id=(peers[order[0]][step],), device_id_type=MESH)
            for g, order, span, _ in self.groups:
                lanes = pl.ds(*span)
                axis = order[1]
                for step in (1, 2, 3):
                    if t >= 2:
                        pl.semaphore_wait(free_sem.at[1, par, self.part, g, step - 1], 1)
                    self.send(self.plane_at({order[0]: pos[order[0]], axis: near[axis][step]}, span), lambda step=step, lanes=lanes: rs3.at[par, step - 1, :, :, lanes], peers[axis][step])

        def phase_4(self):
            t, par = self.t, self.par
            self.drain()
            for g, order, span, _ in self.groups:
                lanes = pl.ds(*span)
                where = (t,) + region({order[0]: pos[order[0]], order[1]: pos[order[1]]}, span)
                plane[where] = plane[where] + (rs3[par, 0, :, :, lanes] + rs3[par, 1, :, :, lanes] + rs3[par, 2, :, :, lanes])
                if t < 2:
                    for step in (1, 2, 3):
                        pl.semaphore_signal(free_sem.at[1, par, self.part, g, step - 1], inc=1, device_id=(peers[order[1]][RING - step],), device_id_type=MESH)
            for g, order, span, _ in self.groups:
                lanes = pl.ds(*span)
                axis = order[2]
                fixed = {order[0]: pos[order[0]], order[1]: pos[order[1]]}
                for step in (1, 2, 3):
                    self.send(self.plane_at({**fixed, axis: near[axis][step]}, span), lambda step=step, lanes=lanes: rs4.at[t, step - 1, :, lanes], peers[axis][step])

        def phase_5(self):
            t = self.t
            self.drain()
            lanes = slice(HALF * self.part, HALF * (self.part + 1))
            block = plane[t, pos[0], pos[1], pos[2], :, lanes] + (rs4[t, 0, :, lanes] + rs4[t, 1, :, lanes] + rs4[t, 2, :, lanes])
            if self.part == 0:
                grad_x[t, core] = block
                self.send(lambda: grad_x.at[t, core], lambda: grad_x.at[t, core], partner)
            else:
                s, l = self.stage, self.layer
                grad = jnp.concatenate([block[:, 0:DIM], block[:, DIM:HALF]], axis=0)
                new = adam_update(acc_down[s, l], grad, master_down[s, l], m1_down[s, l], m2_down[s, l])
                for i in range(3):
                    out_states[2 * i + 1][s, l] = new[i]
                gath[t, core, pos[0], pos[1], pos[2], :, DIM:HALF] = new[0].astype(jnp.bfloat16)
                self.spread()

        def phase_6(self):
            t, s, l = self.t, self.stage, self.layer
            self.drain()
            low = jnp.concatenate([grad_x[t, 0, 0:RING, :], grad_x[t, 1, 0:RING, :]], axis=1)
            high = jnp.concatenate([grad_x[t, 0, RING:SUB, :], grad_x[t, 1, RING:SUB, :]], axis=1)
            grad_up = jnp.where(core == 0, low, high)
            new_up = adam_update(acc_up[s, l], grad_up, master_up[s, l], m1_up[s, l], m2_up[s, l])
            for i in range(3):
                out_states[2 * i][s, l] = new_up[i]
            left, right = new_up[0][:, 0:HALF], new_up[0][:, HALF:FF]
            part_x[t, core] = jnp.where(core == 0, left, right)
            part_x[t, 2] = jnp.where(core == 0, right, left)
            self.send(lambda: part_x.at[t, 2], lambda: part_x.at[t, core], partner)

        def phase_7(self):
            t = self.t
            self.drain()
            block8[t, 0:RING, :] = part_x[t, 0]
            block8[t, RING:SUB, :] = part_x[t, 1]
            rows = jnp.concatenate([block8[t, :, 0:DIM], block8[t, :, DIM:HALF]], axis=0)
            gath[t, core, pos[0], pos[1], pos[2], :, 0:DIM] = rows.astype(jnp.bfloat16)
            self.spread()

        def spread(self):
            for g, order, _, span in self.groups:
                where = self.gath_at({0: pos[0], 1: pos[1], 2: pos[2]}, span)
                for step in (1, 2, 3):
                    self.send(where, where, peers[order[2]][step])

        def phase_8(self):
            self.drain()
            for g, order, _, span in self.groups:
                where = self.gath_at({order[0]: pos[order[0]], order[1]: pos[order[1]]}, span)
                for step in (1, 2, 3):
                    self.send(where, where, peers[order[1]][step])

        def phase_9(self):
            self.drain()
            for g, order, _, span in self.groups:
                where = self.gath_at({order[0]: pos[order[0]]}, span)
                for step in (1, 3):
                    self.send(where, where, peers[order[0]][step])

        def phase_10(self):
            self.drain()
            for g, order, _, span in self.groups:
                axis, half = order[0], half_dim(order[0])
                for way, step in ((0, 1), (1, 3)):
                    where = self.gath_at({axis: near[axis][RING - step], half: pl.ds(2 * way, 2)}, span)
                    self.send(where, where, peers[axis][step])

        def phase_11(self):
            self.drain()
            lanes = pl.ds(DIM * self.part, DIM)
            whole = lambda: gath.at[self.t, core, :, :, :, :, lanes]
            self.send(whole, whole, partner)

        def phase_12(self):
            self.drain()

    chains = [[Chain(t, part) for part in range(2)] for t in range(RING)]
    agenda = sorted((TILES * (t + 1) - 1 + offset + (GATHER_LAG * (3 - t) if phase > 5 else 0), t, part, phase + 1) for t in range(RING) for part in range(2) for phase, offset in enumerate(OFFSETS[part]) if offset is not None)
    finished = set()

    def advance(now):
        while agenda and agenda[0][0] <= now:
            _, t, part, phase = agenda.pop(0)
            chains[t][part].run(phase)
            finished.add((t, part, phase))

    def backward(t):
        s, l = TASKS[t]
        slot = t % 2
        x_copy(t).wait()
        if l == 1:
            cot_copy(s).wait()
            total[...] = jnp.zeros_like(total)

        def fetch(i):
            for copy in weight_copies(t, i):
                copy.wait()

        def front(i, m):
            rows = pl.ds(m * CHUNK, CHUNK)
            h = mm(xbuf[slot, rows, :], wu[i], 1, 0)
            grad_act = mm(cot[s, rows, :], wd[i], 1, 1)
            square = h * h
            tanh = jnp.tanh(h * (GELU_A + GELU_B * square))
            gate = 0.5 * tanh + 0.5
            act_buf[lax.rem(i, 2), rows, :] = (h * gate).astype(jnp.bfloat16)
            slope = gate + (0.5 * h) * (1.0 - tanh * tanh) * (GELU_A + 3.0 * GELU_B * square)
            grad_buf[lax.rem(i, 2), rows, :] = (grad_act * slope).astype(jnp.bfloat16)

        def back_down(i, n):
            j = tile_of(i)
            lanes = pl.ds(n * WIDTH, WIDTH)
            down = mm(act_buf[lax.rem(i, 2)], cot[s, :, lanes], 0, 0).reshape(SUB, 2, ROWS, WIDTH)
            own = jnp.where(core == 0, down[:, 0], down[:, 1])
            other = jnp.where(core == 0, down[:, 1], down[:, 0]).astype(jnp.bfloat16)
            rows = pl.ds(2 * lax.rem(j, 2), 2)
            for h in range(2):
                plane[t, lax.div(j, 2), rows, :, :, pl.ds(HALF + h * DIM + n * WIDTH, WIDTH)] = own[:, h * SUB:(h + 1) * SUB].reshape(2, RING, SUB, WIDTH)
            for k in range(SUB):
                gath[t, 1, 2 + lax.div(j, RING), lax.rem(j, RING), k // 2, :, pl.ds(k % 2 * DIM + n * WIDTH, WIDTH)] = other[k]

        def back_up(i, n, mine):
            up = mm(xbuf[slot, :, pl.ds(n * WIDTH, WIDTH)], grad_buf[lax.rem(i, 2)], 0, 0)
            cols = pl.ds(pl.multiple_of(lax.rem(tile_of(i), RING) * WIDTH, WIDTH), WIDTH)
            if mine:
                plane[t, pl.ds(2 * n, 2), :, :, :, cols] = up.reshape(2, RING, RING, SUB, WIDTH)
            else:
                gath[t, 1, n, :, :, :, cols] = up.astype(jnp.bfloat16).reshape(RING, RING, ROWS, WIDTH)

        def back_dx(i, m):
            rows = pl.ds(m * CHUNK, CHUNK)
            total[rows, :] = total[rows, :] + mm(grad_buf[lax.rem(i, 2), rows, :], wu[i], 1, 1)

        def events(k):
            if k == 3:
                for chain in chains[t]:
                    chain.early()
            if k == TILES - 1:
                for chain in chains[t]:
                    chain.late()
            advance(TILES * t + k)

        def tile(i, mine, ahead):
            if ahead:
                fetch(i + 1)
            for m in range(HALF // CHUNK):
                if ahead:
                    front(i + 1, m)
                for n in range(2):
                    if m == n * (HALF // CHUNK // 2):
                        back_down(i, n)
                        back_up(i, n, mine)
                if l == 1:
                    back_dx(i, m)
            if t < 3:
                for copy in weight_copies(t + 1, i):
                    copy.start()

        def segment(start, stop, mine):
            def body(i, carry):
                tile(i, mine, True)
                for k in range(start, stop):
                    if k == 3 or agenda and agenda[0][0] <= TILES * t + k:
                        @pl.when(i == k)
                        def _():
                            events(k)
                return carry

            lax.fori_loop(start, stop, body, 0)

        fetch(0)
        for m in range(HALF // CHUNK):
            front(0, m)
        segment(0, RING, False)
        segment(RING, TILES - 1, True)
        tile(TILES - 1, True, False)
        events(TILES - 1)
        if l == 1:
            cot[s] = (cot[s].astype(jnp.float32) + total[...]).astype(jnp.bfloat16)
        if t < 2:
            x_copy(t + 2).start()
        else:
            next_copy(t - 2).start()

    def forward(t, s, l, now):
        if l == 0:
            next_copy(s).wait()
        total[...] = jnp.zeros_like(total)

        def body(i, carry):
            half, lane = lax.div(i, 2), lax.rem(i, 2)
            lanes = pl.ds(pl.multiple_of(lane * WIDTH, WIDTH), WIDTH)
            raw = gath[t, half, :, :, :, :, lanes].astype(jnp.float32).reshape(RING ** 3, ROWS, WIDTH)
            ups, downs = [], []
            for q in range(2):
                ups.append(raw[:, q * SUB:(q + 1) * SUB].reshape(DIM, WIDTH).astype(jnp.bfloat16))
                rows = pl.ds(2 * lane, 2)
                even = gath[t, 0, 2 * half + q, rows, :, :, DIM:HALF].reshape(SUB, 1, ROWS, DIM)
                odd = gath[t, 1, 2 * half + q, rows, :, :, DIM:HALF].reshape(SUB, 1, ROWS, DIM)
                downs.append(jnp.concatenate([even, odd], axis=1).reshape(WIDTH, DIM))
            w1, w2 = jnp.concatenate(ups, axis=1), jnp.concatenate(downs, axis=0)
            count = HALF // SPAN
            hidden = mm(xbuf[s, 0:SPAN, :], w1, 1, 0)
            for m in range(count):
                h = hidden
                if m + 1 < count:
                    hidden = mm(xbuf[s, pl.ds((m + 1) * SPAN, SPAN), :], w1, 1, 0)
                tanh = jnp.tanh(h * (GELU_A + GELU_B * (h * h)))
                act = (h * (0.5 * tanh + 0.5)).astype(jnp.bfloat16)
                span = pl.ds(m * SPAN, SPAN)
                total[span, :] = total[span, :] + mm(act, w2, 1, 0)
            for k in range(RING):
                if agenda and agenda[0][0] <= now + k:
                    @pl.when(i == k)
                    def _():
                        advance(now + k)
            return carry

        lax.fori_loop(0, RING, body, 0)
        xbuf[s] = (xbuf[s].astype(jnp.float32) + total[...]).astype(jnp.bfloat16)
        if l == 1:
            y_copy(s).start()
        return now + RING

    for t in range(RING):
        backward(t)
    now = RING * TILES - 1
    for t, s, l in FORWARD:
        while not finished >= {(t, 0, 12), (t, 1, 12)}:
            now = max(now, agenda[0][0])
            advance(agenda[0][0])
        now = forward(t, s, l, now)
    for s in range(2):
        y_copy(s).wait()


def fused_step(*args):
    vmem = pl.BlockSpec(memory_space=pltpu.VMEM)
    hbm = pl.BlockSpec(memory_space=pl.ANY)
    up_state = jax.ShapeDtypeStruct(args[5].shape, jnp.float32)
    down_state = jax.ShapeDtypeStruct(args[6].shape, jnp.float32)
    scratch = [
        pltpu.VMEM((TILES, DIM, WIDTH), jnp.bfloat16),
        pltpu.VMEM((TILES, WIDTH, DIM), jnp.bfloat16),
        pltpu.VMEM((2, HALF, DIM), jnp.bfloat16),
        pltpu.VMEM((2, HALF, DIM), jnp.bfloat16),
        pltpu.VMEM((HALF, DIM), jnp.float32),
        pltpu.VMEM((2, HALF, WIDTH), jnp.bfloat16),
        pltpu.VMEM((2, HALF, WIDTH), jnp.bfloat16),
        pltpu.VMEM((RING,) * RING + (SUB, FF), jnp.float32),
        pltpu.VMEM((2, 2, 2, RING, SUB, FF), jnp.float32),
        pltpu.VMEM((2, 2, RING, RING, SUB, FF), jnp.float32),
        pltpu.VMEM((2, 3, RING, SUB, FF), jnp.float32),
        pltpu.VMEM((RING, 3, SUB, FF), jnp.float32),
        pltpu.VMEM((RING, 2, SUB, HALF), jnp.float32),
        pltpu.VMEM((RING, 3, RING, HALF), jnp.float32),
        pltpu.VMEM((RING, SUB, HALF), jnp.float32),
        pltpu.VMEM((RING, 2, RING, RING, RING, ROWS, HALF), jnp.bfloat16),
        pltpu.SemaphoreType.DMA((2, TILES)),
        pltpu.SemaphoreType.DMA((6,)),
        pltpu.SemaphoreType.DMA((SUB, 9)),
        pltpu.SemaphoreType.DMA((SUB, 66)),
        pltpu.SemaphoreType.REGULAR((2, 2, 2, 3, 3)),
    ]
    return pl.pallas_call(
        step_kernel,
        out_shape=(up_state, down_state) * 3 + (jax.ShapeDtypeStruct(args[2].shape, jnp.bfloat16),),
        in_specs=[hbm] * 5 + [vmem] * SUB,
        out_specs=(vmem,) * 6 + (hbm,),
        scratch_shapes=scratch,
        compiler_params=pltpu.CompilerParams(collective_id=0, has_side_effects=True, vmem_limit_bytes=67043328),
        name='step',
    )(*args)


def finish_kernel(*refs):
    count = len(refs) // 3
    sources, results, stage, sem = refs[:count], refs[count:2 * count], refs[2 * count:3 * count], refs[3 * count]
    inward = [pltpu.make_async_copy(sources[i], stage[i], sem.at[0, i]) for i in range(count)]
    outward = [pltpu.make_async_copy(stage[i], results[i], sem.at[1, i]) for i in range(count)]
    for copy in inward:
        copy.start()
    for i in range(count):
        inward[i].wait()
        outward[i].start()
    for copy in outward:
        copy.wait()


def finish(parts):
    hbm = pl.BlockSpec(memory_space=pl.ANY)
    return pl.pallas_call(
        finish_kernel,
        out_shape=tuple(jax.ShapeDtypeStruct(part.shape, part.dtype) for part in parts),
        in_specs=[hbm] * len(parts),
        out_specs=(hbm,) * len(parts),
        scratch_shapes=[pltpu.VMEM(part.shape, part.dtype) for part in parts] + [pltpu.SemaphoreType.DMA((2, len(parts)))],
        name='finish',
    )(*parts)


def solution(mesh):
    tok_spec = P(None, 'fsdp')
    layer_spec = P(None, None, 'fsdp')
    rep_spec = P()

    def device_step(*args):
        return tuple(finish(fused_step(*args)))

    return jax.shard_map(device_step, mesh=mesh, in_specs=(layer_spec, tok_spec, tok_spec, rep_spec, rep_spec) + (layer_spec,) * SUB, out_specs=(layer_spec,) * 6 + (tok_spec,), check_vma=False)
```
